32 devices in a mesh: half: 2 (over core), row: 4 (over y, x), col: 4 (over z).
Axes of the slice: x: 2, y: 2, z: 4, core: 2. Of those that a mesh axis runs over, the one named last changes fastest.
Arguments:
- particles: bfloat16 [64, 2, 64, 4096], P(('half', 'row', 'col')), may hold values from -9 to 9
- orient_bin: int32 [64], P(('half', 'row', 'col')), may hold values from 0 to 15
- tilt_slope: int32 [64, 2], P(('half', 'row', 'col')), may hold values from 12 to 40
- interp_table: bfloat16 [16, 3, 64, 64], replicated, may hold values from 0 to 1.6, as said below
Outputs:
- half_maps: float32 [2, 2, 64, 4096], P('half', None, 'row', 'col')
- shell_power: float32 [2, 29], replicated
- shell_correlation: float32 [2, 29], P('half')
The draws below stay inside these ranges and needn't reach their ends.
Inputs may be any that keep to these rules, and one draw needn't show every extreme that they name: `interp_table`: nonnegative entries.
All inputs are finite; a program needn't handle non-finite values.
Results may differ from the reference program's by a relative error of at most 0.00063.
Values sent between devices are 32-bit elements; how exact they have to be, the bound alone decides.
A program may use at most 64 MiB of HBM per device.

```python
import jax
import jax.numpy as jnp
from jax import lax

GRID = 64
BINS = 16
SHELLS = 29
PARTICLES = 64


def draw_particles(key, part):
    full_shape = (PARTICLES, 2, GRID, GRID * GRID)
    signal = jax.random.normal(jax.random.fold_in(key, 11), (1, 2, GRID, GRID * GRID), jnp.float32)
    noise_part = jax.random.normal(key, full_shape, jnp.float32)
    combined = 0.7 * signal + noise_part
    return jnp.clip(combined, -9.0, 9.0).astype(jnp.bfloat16)


def draw_interp_table(key, part):
    full_shape = (BINS, 3, GRID, GRID)
    row_index = jnp.arange(GRID)[:, None]
    col_index = jnp.arange(GRID)[None, :]
    offset = jnp.abs(row_index - col_index)
    key_diagonal = jax.random.fold_in(key, 21)
    key_band = jax.random.fold_in(key, 22)
    key_dense = jax.random.fold_in(key, 23)
    diagonal_part = jax.random.uniform(key_diagonal, full_shape, jnp.float32, 0.8, 1.2)
    band_part = jax.random.uniform(key_band, full_shape, jnp.float32, 0.03, 0.25)
    dense_part = jax.random.uniform(key_dense, full_shape, jnp.float32, 0.0, 0.02)
    table = jnp.where(offset == 0, diagonal_part, jnp.where(offset <= 2, band_part, 0.0)) + dense_part
    return table.astype(jnp.bfloat16)


def set_ends(result, stream_key, least, high):
    index_at = [jax.random.randint(jax.random.fold_in(stream_key, axis), (), 0, length) for axis, length in enumerate(result.shape)]
    main_axis = result.shape.index(max(result.shape))
    beside = index_at[:main_axis] + [(index_at[main_axis] + 1) % result.shape[main_axis]] + index_at[main_axis + 1:]
    return result.at[tuple(index_at)].set(least).at[tuple(beside)].set(high)


def setup_inputs(seed: int = 0) -> dict:
    keys = jax.random.split(jax.random.key(seed), 5)
    particles = draw_particles(jax.random.fold_in(keys[4], 71), 0)
    orient_bin = set_ends(jax.random.randint(keys[1], (PARTICLES,), 0, BINS), jax.random.fold_in(keys[1], 1), 0, BINS - 1).astype(jnp.int32)
    tilt_slope = set_ends(jax.random.randint(keys[2], (PARTICLES, 2), 12, 41), jax.random.fold_in(keys[2], 1), 12, 40).astype(jnp.int32)
    interp_table = draw_interp_table(jax.random.fold_in(keys[4], 71), 0)
    return dict(particles=particles, orient_bin=orient_bin, tilt_slope=tilt_slope, interp_table=interp_table)


def wedge_mask(tilt_limits, grid_size):
    centre = grid_size // 2
    wave_first = (jnp.arange(grid_size, dtype=jnp.int32) - centre)[:, None]
    wave_third = (jnp.arange(grid_size * grid_size, dtype=jnp.int32) % grid_size - centre)[None, :]
    tilt_limit = jnp.where(wave_first * wave_third >= 0, tilt_limits[0], tilt_limits[1])
    inside = 16 * jnp.abs(wave_third) <= tilt_limit * jnp.abs(wave_first)
    return inside.astype(jnp.float32)

def interpolate(stacked, kernels, grid_size):
    components = stacked.shape[0]
    kernels = kernels.astype(jnp.float32)
    along_first = jnp.einsum('ax,cxm->cam', kernels[0], stacked.astype(jnp.float32), precision=lax.Precision.HIGHEST).astype(jnp.bfloat16)
    along_first = along_first.reshape(components, grid_size, grid_size, grid_size)
    along_second = jnp.einsum('by,cayz->cabz', kernels[1], along_first.astype(jnp.float32), precision=lax.Precision.HIGHEST).astype(jnp.bfloat16)
    along_third = jnp.einsum('dz,cabz->cabd', kernels[2], along_second.astype(jnp.float32), precision=lax.Precision.HIGHEST)
    return along_third.reshape(components, grid_size, grid_size * grid_size)

def reference(particles, orient_bin, tilt_slope, interp_table):
    grid_size = GRID
    half_labels = (jnp.arange(PARTICLES, dtype=jnp.int32) // (PARTICLES // 2)).astype(jnp.int32)

    def insert_one(partial_value, inputs):
        volume_data, bin_row, tilt_limits, half_label = inputs
        weight = wedge_mask(tilt_limits, grid_size)
        stacked = jnp.stack([volume_data[0] * weight, volume_data[1] * weight, weight]).astype(jnp.bfloat16)
        kernels = interp_table[bin_row]
        inserted = interpolate(stacked, kernels, grid_size)
        partial_value = partial_value.at[half_label].add(inserted)
        return (partial_value, None)
    partial_value = jnp.zeros((2, 3, grid_size, grid_size * grid_size), jnp.float32)
    partial_value, unused_out = lax.scan(insert_one, partial_value, (particles, orient_bin, tilt_slope, half_labels))
    half_maps = partial_value[:, :2] / (partial_value[:, 2:3] + 1.0)
    centre = grid_size // 2
    wave_first = (jnp.arange(grid_size, dtype=jnp.int32) - centre)[:, None]
    plane_index = jnp.arange(grid_size * grid_size, dtype=jnp.int32)[None, :]
    wave_second = plane_index // grid_size - centre
    wave_third = plane_index % grid_size - centre
    radius_sq = (wave_first * wave_first + wave_second * wave_second + wave_third * wave_third).reshape(-1)
    bounds = jnp.arange(4, centre, dtype=jnp.int32)
    shell_index = lax.optimization_barrier(jnp.sum((radius_sq[:, None] >= (bounds * bounds)[None, :]).astype(jnp.int32), axis=1)).astype(jnp.int32)
    shell_index = jnp.where(radius_sq < centre * centre, shell_index, SHELLS).astype(jnp.int32)
    map_first = half_maps[0]
    map_second = half_maps[1]
    cross_term = (map_first[0] * map_second[0] + map_first[1] * map_second[1]).reshape(-1)
    power_first = (map_first[0] * map_first[0] + map_first[1] * map_first[1]).reshape(-1)
    power_second = (map_second[0] * map_second[0] + map_second[1] * map_second[1]).reshape(-1)

    def shell_sum(values):
        return jax.ops.segment_sum(values, shell_index, num_segments=SHELLS + 1)[:SHELLS]
    cross_sum = shell_sum(cross_term)
    first_sum = shell_sum(power_first)
    second_sum = shell_sum(power_second)
    counts = shell_sum(jnp.ones_like(cross_term))
    shell_power = jnp.stack([first_sum, second_sum]) / counts[None, :]
    correlation = cross_sum / jnp.sqrt(first_sum * second_sum + 1e-06)
    shell_correlation = jnp.stack([correlation, correlation])
    return (half_maps, shell_power, shell_correlation)
```

```python
import functools

import jax
import jax.numpy as jnp
import numpy as np
from jax import lax
from jax.experimental import pallas as pl
from jax.experimental.pallas import tpu as pltpu
from jax.sharding import PartitionSpec as P

F32 = jnp.float32
BF16 = jnp.bfloat16
LANES = 128
VMEM_LIMIT = 60 * 1024 * 1024
FINISH_LIMIT = 4 * 1024 * 1024
MESH = pl.DeviceIdType.MESH


def dot_nt(left, right):
    return lax.dot_general(left, right, (((1,), (1,)), ((), ())), preferred_element_type=F32)


def dot_nn(left, right):
    return lax.dot_general(left, right, (((1,), (0,)), ((), ())), preferred_element_type=F32)


def block_diagonal(block, copies):
    zero = jnp.zeros_like(block)
    rows = [
        jnp.concatenate([block if i == j else zero for j in range(copies)], axis=1)
        for i in range(copies)
    ]
    return jnp.concatenate(rows, axis=0)


def wedge_mask(limit_same, limit_other, grid, lanes):
    centre = grid // 2
    first = lax.broadcasted_iota(jnp.int32, (grid, lanes), 0) - centre
    third = lax.broadcasted_iota(jnp.int32, (grid, lanes), 1) % grid - centre
    limit = jnp.where(first * third >= 0, limit_same, limit_other)
    inside = 16 * jnp.abs(third) <= limit * jnp.abs(first)
    return jnp.where(inside, 1.0, 0.0).astype(BF16)


def shell_counts(grid):
    centre = grid // 2
    wave = np.arange(grid) - centre
    square = wave * wave
    radius = square[:, None, None] + square[None, :, None] + square[None, None, :]
    shell = np.sum([radius >= k * k for k in range(4, centre)], axis=0)
    return np.bincount(shell[radius < centre * centre], minlength=centre - 3)


def kernel(
    dims,
    bins_hbm, tilt_hbm, part_hbm, table_hbm,
    maps_ref, spectra_ref,
    part_ref, table_ref, bins_ref, tilt_ref, stage_a, stage_b, sums, rows_in, cols_in, other_map,
    third_ref, numbers, numbers_in, numbers_s, slab_first, slab_second, wide_second,
    bin_first, bin_second, bin_third, weight,
    stats, stats_in, total,
    send_row, recv_row, send_col, recv_col, send_num, recv_num, copy_num,
    send_stat, recv_stat, send_half, recv_half, load_part, load_table, load_bins, load_tilt,
):
    grid, particles, R, C, pitch, bins = dims
    N = R * C
    rl, bl = grid // R, grid // C
    phases = R.bit_length() - 1
    half, row, col = lax.axis_index("half"), lax.axis_index("row"), lax.axis_index("col")
    me = row * C + col

    def peer_id(step):
        peer = (me + step) % N
        return {"row": peer // C, "col": peer % C}

    def power_of(phase):
        low, high = 2 ** (phase % phases), 2 ** ((phase + 1) % phases)
        return low + half * (high - low)

    def row_partner(phase):
        weight_of = power_of(phase)
        bit = (row // weight_of) % 2
        return {"row": row + (1 - 2 * bit) * weight_of}

    def slab_of(index):
        slab = row
        for phase in range(phases):
            if (index >> (phases - 1 - phase)) & 1:
                weight_of = power_of(phase)
                bit = (row // weight_of) % 2
                slab = slab + (1 - 2 * bit) * weight_of
        return slab

    bins_load = pltpu.make_async_copy(bins_hbm, bins_ref, load_bins)
    tilt_load = pltpu.make_async_copy(tilt_hbm, tilt_ref, load_tilt)
    bins_load.start()
    tilt_load.start()
    table_load = pltpu.make_async_copy(table_hbm, table_ref, load_table)
    table_load.start()
    part_loads = [
        pltpu.make_async_copy(part_hbm.at[p], part_ref.at[p], load_part.at[p])
        for p in range(particles)
    ]
    for copy in part_loads:
        copy.start()

    barrier = pltpu.get_barrier_semaphore()
    for step in range(1, N):
        pl.semaphore_signal(barrier, inc=1, device_id=peer_id(step), device_id_type=MESH)
    pl.semaphore_signal(barrier, inc=1, device_id={"half": 1 - half}, device_id_type=MESH)

    bins_load.wait()
    tilt_load.wait()
    lane = lax.broadcasted_iota(jnp.int32, (1, LANES), 1)
    packed = jnp.zeros((1, LANES), jnp.int32)
    for p in range(particles):
        for i, value in enumerate((bins_ref[p], tilt_ref[p, 0], tilt_ref[p, 1])):
            packed = jnp.where(lane == 3 * p + i, value, packed)
    numbers[0] = packed
    numbers_in[me] = packed

    table_load.wait()
    firsts_, seconds_ = [], []
    for p in range(particles):
        bin_row = bins_ref[p]
        first = table_ref[bin_row, 0].astype(F32)
        second = table_ref[bin_row, 1].astype(F32)
        for r in range(R):
            slab_first[p, r] = first[r * rl:(r + 1) * rl]
        for q in range(C):
            slab_second[p, q] = second[q * bl:(q + 1) * bl]
        firsts_.append(
            jnp.concatenate([slab_first[p, slab_of(j)] for j in range(R)], axis=0).astype(BF16)
        )
        seconds_.append(jnp.concatenate(
            [slab_second[p, (col + 1 + k) % C] for k in range(C)], axis=0
        ).astype(BF16))
        third_ref[p * LANES:(p + 1) * LANES, :] = block_diagonal(table_ref[bin_row, 2].T, 2)

    low_lanes = lax.broadcasted_iota(jnp.int32, (grid, LANES), 1) < grid
    for p in range(particles):
        first = firsts_[p]
        mask = wedge_mask(tilt_ref[p, 0], tilt_ref[p, 1], grid, LANES)

        part_loads[p].wait()
        for at in range(grid // 2):
            span = slice(at * LANES, (at + 1) * LANES)
            real, imag = part_ref[p, 0, :, span], part_ref[p, 1, :, span]
            even = jnp.where(low_lanes, real, pltpu.roll(imag, grid, 1)) * mask
            odd = jnp.where(low_lanes, pltpu.roll(real, grid, 1), imag) * mask
            result = dot_nn(first, jnp.concatenate([even, odd], axis=1))
            for o in range(2):
                to = (2 * at + o) * pitch
                stage_a[p, to:to + grid, :] = result[:, o * LANES:(o + 1) * LANES]

    pl.semaphore_wait(barrier, N)
    def all_to(src, dst, send, recv):
        return [
            pltpu.make_async_remote_copy(
                src_ref=src.at[0], dst_ref=dst.at[me], send_sem=send, recv_sem=recv,
                device_id=peer_id(step), device_id_type=MESH,
            )
            for step in range(1, N)
        ]

    def whole(dst, send, recv):
        return pltpu.make_async_remote_copy(
            src_ref=dst.at[pl.ds(0, N - 1)], dst_ref=dst.at[pl.ds(0, N - 1)],
            send_sem=send, recv_sem=recv, device_id=peer_id(1), device_id_type=MESH,
        )

    for copy in all_to(numbers, numbers_in, send_num, recv_num):
        copy.start()

    def row_copy(phase, k):
        keep = R >> (phase + 1)
        return pltpu.make_async_remote_copy(
            src_ref=sums.at[k, pl.ds(keep, keep)],
            dst_ref=rows_in.at[k, pl.ds(keep, keep)],
            send_sem=send_row.at[phase, k], recv_sem=recv_row.at[phase, k],
            device_id=row_partner(phase), device_id_type=MESH,
        )

    def col_copy(k):
        return pltpu.make_async_remote_copy(
            src_ref=sums.at[k, 0], dst_ref=cols_in.at[k],
            send_sem=send_col.at[k], recv_sem=recv_col.at[k],
            device_id={"col": (col + 1 + k) % C}, device_id_type=MESH,
        )

    def along_second(start, stop):
        for p in range(particles):
            second = seconds_[p]
            for a in range(start, stop, 2):
                block = jnp.concatenate(
                    [stage_a[p, pl.ds(a + i, grid, stride=pitch), :] for i in range(2)], axis=1
                ).astype(BF16)
                result = dot_nn(second, block).astype(stage_b.dtype)
                for i in range(2):
                    for k in range(C):
                        stage_b[p, k, a + i] = result[
                            k * bl:(k + 1) * bl, i * LANES:(i + 1) * LANES
                        ]

    def along_third(k, j0, j1):
        count = (j1 - j0) * rl
        block = jnp.concatenate(
            [
                stage_b[p, k, j0 * rl:j1 * rl].reshape(count * bl, LANES)
                for p in range(particles)
            ],
            axis=1,
        ).astype(BF16)
        result = dot_nn(block, third_ref[...])
        for j in range(j0, j1):
            sums[k, j] = result[(j - j0) * rl * bl:(j - j0 + 1) * rl * bl]

    along_second(grid // 2, grid)
    for k in range(C):
        along_third(k, R // 2, R)
        row_copy(0, k).start()
    along_second(0, grid // 2)
    for k in range(C):
        along_third(k, 0, R // 2)

    local = pltpu.make_async_copy(numbers_in, numbers_s, copy_num)
    weight[...] = jnp.zeros_like(weight)
    ones = jnp.ones((grid, LANES), BF16)

    def bin_tables(n, carry):
        first = table_ref[n, 0].astype(F32)
        second = dot_nn(table_ref[n, 1], ones)
        for r in range(R):
            slab_first[0, r] = first[r * rl:(r + 1) * rl]
        for q in range(C):
            wide_second[q] = second[q * bl:(q + 1) * bl]
        bin_first[n] = slab_first[0, row]
        bin_second[n] = wide_second[col]
        across = table_ref[n, 2].T
        bin_third[n] = jnp.concatenate([across, across], axis=1)
        return carry

    lax.fori_loop(0, bins, bin_tables, 0, unroll=4)

    together = 2
    first_wave = lax.broadcasted_iota(jnp.int32, (grid, LANES), 0) - grid // 2
    third_wave = lax.broadcasted_iota(jnp.int32, (grid, LANES), 1) % grid - grid // 2
    same_side = first_wave * third_wave >= 0
    first_size, third_size = jnp.abs(first_wave), 16 * jnp.abs(third_wave)
    low_rows = lax.broadcasted_iota(jnp.int32, (rl, LANES), 1) < grid
    low_seconds = lax.broadcasted_iota(jnp.int32, (bl, LANES), 1) < grid

    def add_weight(step, carry):
        members = [(step * together + n, p) for n in range(together) for p in range(particles)]
        blocks, thirds = [], []
        for i in range(0, len(members), 2):
            numbers_of = [
                [numbers_s[n, 0, 3 * p + v] for v in range(3)] for n, p in members[i:i + 2]
            ]
            limit = jnp.where(
                same_side,
                jnp.where(low_lanes, numbers_of[0][1], numbers_of[1][1]),
                jnp.where(low_lanes, numbers_of[0][2], numbers_of[1][2]),
            )
            mask = jnp.where(third_size <= limit * first_size, 1.0, 0.0).astype(BF16)
            along = [dot_nn(bin_first[value[0]].astype(BF16), mask) for value in numbers_of]
            first = jnp.where(low_rows, along[0], along[1]).astype(BF16).astype(F32)
            second = jnp.where(
                low_seconds, bin_second[numbers_of[0][0]], bin_second[numbers_of[1][0]]
            )
            blocks.append(
                jnp.concatenate([first[a:a + 1] * second for a in range(rl)], axis=0).astype(BF16)
            )
            thirds += [bin_third[value[0]] for value in numbers_of]
        weight[...] += dot_nn(jnp.concatenate(blocks, axis=1), jnp.concatenate(thirds, axis=0))
        return carry

    share = N // together // C
    for step in range(C + phases):
        for phase in range(phases):
            k = step - phase
            if 0 <= k < C:
                keep = R >> (phase + 1)
                row_copy(phase, k).wait_recv()
                sums[k, :keep] = sums[k, :keep] + rows_in[k, keep:2 * keep]
                if phase + 1 < phases:
                    row_copy(phase + 1, k).start()
                elif k < C - 1:
                    col_copy(k).start()
        if step == 0:
            whole(numbers_in, send_num, recv_num).wait_recv()
            local.start()
            local.wait()
        if step < C:
            lax.fori_loop(step * share, (step + 1) * share, add_weight, 0)

    for k in range(C - 1):
        col_copy(k).wait_recv()
    block = sums[C - 1, 0]
    for k in range(C - 1):
        block = block + cols_in[k]
    weight[...] = block / (weight[...] + 1.0)
    low = lax.broadcasted_iota(jnp.int32, (rl, LANES), 1) < grid
    for pair in range(bl // 2):
        span = slice(pair * LANES, (pair + 1) * LANES)
        even, odd = (weight[pl.ds(2 * pair + i, rl, stride=bl), :] for i in range(2))
        maps_ref[0, 0, :, span] = jnp.where(low, even, pltpu.roll(odd, grid, 1))
        maps_ref[0, 1, :, span] = jnp.where(low, pltpu.roll(even, grid, 1), odd)

    half_copy = pltpu.make_async_remote_copy(
        src_ref=maps_ref.at[0], dst_ref=other_map, send_sem=send_half, recv_sem=recv_half,
        device_id={"half": 1 - half}, device_id_type=MESH,
    )
    half_copy.start()
    for k in range(C):
        for phase in range(phases):
            row_copy(phase, k).wait_send()
    for k in range(C - 1):
        col_copy(k).wait_send()
    whole(numbers_in, send_num, recv_num).wait_send()

    centre = grid // 2
    shells = centre - 3
    tile_rows = lax.broadcasted_iota(jnp.int32, (rl, LANES), 0)
    tile_lanes = lax.broadcasted_iota(jnp.int32, (rl, LANES), 1)
    wave_first = row * rl + tile_rows - centre
    wave_third = tile_lanes % grid - centre
    fixed = wave_first * wave_first + wave_third * wave_third
    radius = []
    for pair in range(bl // 2):
        wave_second = col * bl + 2 * pair + tile_lanes // grid - centre
        radius.append(fixed + wave_second * wave_second)
    stats[...] = jnp.zeros_like(stats)

    def shell_sums(rows_at, values):
        for s in range(shells):
            least = (s + 3) * (s + 3) if s else 0
            beyond = (s + 4) * (s + 4)
            parts = [jnp.zeros((rl, LANES), F32) for _ in values]
            for pair, r2 in enumerate(radius):
                inside = (r2 >= least) & (r2 < beyond)
                parts = [
                    part + jnp.where(inside, value[pair], 0.0)
                    for part, value in zip(parts, values)
                ]
            for at, part in zip(rows_at, parts):
                stats[pl.ds(at + s, 1), :] = jnp.sum(part, axis=0, keepdims=True)

    def tiles(ref, c):
        return [ref[c, :, pair * LANES:(pair + 1) * LANES] for pair in range(bl // 2)]

    mine = [tiles(maps_ref.at[0], c) for c in range(2)]
    shell_sums([32 + 32 * half], [[x * x + y * y for x, y in zip(*mine)]])
    half_copy.wait()
    theirs = [tiles(other_map, c) for c in range(2)]
    mine = [tiles(maps_ref.at[0], c) for c in range(2)]
    shell_sums(
        [0, 64 - 32 * half],
        [
            [x * u + y * v for x, y, u, v in zip(*mine, *theirs)],
            [u * u + v * v for u, v in zip(*theirs)],
        ],
    )
    mine = jnp.sum(stats[...].T, axis=0, keepdims=True)
    total[0] = mine
    stats_in[me] = mine
    for copy in all_to(total, stats_in, send_stat, recv_stat):
        copy.start()
    whole(stats_in, send_stat, recv_stat).wait()
    spectra = stats_in[0]
    for n in range(1, N):
        spectra = spectra + stats_in[n]
    spectra_ref[...] = spectra


def finish(shells, maps_in_ref, spectra_ref, counts_ref, maps_ref, power_ref, corr_ref):
    maps_ref[...] = maps_in_ref[...]
    spectra = spectra_ref[...]
    cross = spectra[:, 0:shells]
    power_first = spectra[:, 32:32 + shells]
    power_second = spectra[:, 64:64 + shells]
    power_ref[0:1, :] = power_first / counts_ref[...]
    power_ref[1:2, :] = power_second / counts_ref[...]
    corr_ref[...] = cross / jnp.sqrt(power_first * power_second + 1e-6)


def solution(mesh):
    R, C = mesh.shape["row"], mesh.shape["col"]
    N = R * C

    def local(particles, orient_bin, tilt_slope, interp_table):
        count, _, grid, plane = particles.shape
        rl, cl, bl = grid // R, plane // C, grid // C
        shells = grid // 2 - 3
        phases = R.bit_length() - 1
        pitch = grid + 8
        bins = interp_table.shape[0]
        counts = jnp.asarray(shell_counts(grid)[None], F32)
        vmem, hbm = pl.BlockSpec(memory_space=pltpu.VMEM), pl.BlockSpec(memory_space=pltpu.HBM)
        dma = pltpu.SemaphoreType.DMA
        maps, spectra = pl.pallas_call(
            functools.partial(kernel, (grid, count, R, C, pitch, bins)),
            out_shape=(
                pltpu.VMEM((1, 2, rl, cl), F32),
                pltpu.VMEM((1, LANES), F32),
            ),
            in_specs=[hbm, hbm, hbm, hbm],
            out_specs=(vmem, vmem),
            scratch_shapes=[
                pltpu.VMEM(particles.shape, particles.dtype),
                pltpu.VMEM(interp_table.shape, interp_table.dtype),
                pltpu.SMEM(orient_bin.shape, jnp.int32),
                pltpu.SMEM(tilt_slope.shape, jnp.int32),
                pltpu.VMEM((count, grid * pitch, LANES), F32),
                pltpu.VMEM((count, C, grid, bl, LANES), F32 if bl % 16 else BF16),
                pltpu.VMEM((C, R, rl * bl, LANES), F32),
                pltpu.VMEM((C, R, rl * bl, LANES), F32),
                pltpu.VMEM((C - 1, rl * bl, LANES), F32),
                pltpu.VMEM((2, rl, cl), F32),
                pltpu.VMEM((count * LANES, LANES), BF16),
                pltpu.VMEM((1, 1, LANES), jnp.int32),
                pltpu.VMEM((N, 1, LANES), jnp.int32),
                pltpu.SMEM((N, 1, LANES), jnp.int32),
                pltpu.VMEM((count, R, rl, grid), F32),
                pltpu.VMEM((count, C, bl, grid), F32),
                pltpu.VMEM((C, bl, LANES), F32),
                pltpu.VMEM((bins, rl, grid), F32),
                pltpu.VMEM((bins, bl, LANES), F32),
                pltpu.VMEM((bins, grid, LANES), BF16),
                pltpu.VMEM((rl * bl, LANES), F32),
                pltpu.VMEM((LANES, LANES), F32),
                pltpu.VMEM((N, 1, LANES), F32),
                pltpu.VMEM((1, 1, LANES), F32),
                dma((phases, C)), dma((phases, C)),
                dma((C - 1,)), dma((C - 1,)),
                dma, dma, dma,
                dma, dma,
                dma, dma, dma((count,)), dma, dma, dma,
            ],
            compiler_params=pltpu.CompilerParams(
                collective_id=0, has_side_effects=True, vmem_limit_bytes=VMEM_LIMIT
            ),
        )(orient_bin, tilt_slope, particles, interp_table)
        return pl.pallas_call(
            functools.partial(finish, shells),
            out_shape=(
                jax.ShapeDtypeStruct((1, 2, rl, cl), F32),
                jax.ShapeDtypeStruct((2, shells), F32),
                jax.ShapeDtypeStruct((1, shells), F32),
            ),
            in_specs=[vmem, vmem, vmem],
            out_specs=(vmem, vmem, vmem),
            compiler_params=pltpu.CompilerParams(vmem_limit_bytes=FINISH_LIMIT),
        )(maps, spectra, counts)

    placed = (
        P(("half", "row", "col"), None, None, None),
        P(("half", "row", "col")),
        P(("half", "row", "col"), None),
        P(),
    )
    return jax.shard_map(
        local,
        mesh=mesh,
        in_specs=placed,
        out_specs=(P("half", None, "row", "col"), P(), P("half", None)),
        check_vma=False,
    )
```

```python
import functools

import jax
import jax.numpy as jnp
import numpy as np
from jax import lax
from jax.experimental import pallas as pl
from jax.experimental.pallas import tpu as pltpu
from jax.sharding import PartitionSpec as P

F32 = jnp.float32
BF16 = jnp.bfloat16
LANES = 128
VMEM_LIMIT = 60 * 1024 * 1024
FINISH_LIMIT = 4 * 1024 * 1024
MESH = pl.DeviceIdType.MESH


def dot_nt(left, right):
    return lax.dot_general(left, right, (((1,), (1,)), ((), ())), preferred_element_type=F32)


def dot_nn(left, right):
    return lax.dot_general(left, right, (((1,), (0,)), ((), ())), preferred_element_type=F32)


def block_diagonal(block, copies):
    zero = jnp.zeros_like(block)
    rows = [
        jnp.concatenate([block if i == j else zero for j in range(copies)], axis=1)
        for i in range(copies)
    ]
    return jnp.concatenate(rows, axis=0)


def wedge_mask(limit_same, limit_other, grid, lanes):
    centre = grid // 2
    first = lax.broadcasted_iota(jnp.int32, (grid, lanes), 0) - centre
    third = lax.broadcasted_iota(jnp.int32, (grid, lanes), 1) % grid - centre
    limit = jnp.where(first * third >= 0, limit_same, limit_other)
    inside = 16 * jnp.abs(third) <= limit * jnp.abs(first)
    return jnp.where(inside, 1.0, 0.0).astype(BF16)


def shell_counts(grid):
    centre = grid // 2
    wave = np.arange(grid) - centre
    square = wave * wave
    radius = square[:, None, None] + square[None, :, None] + square[None, None, :]
    shell = np.sum([radius >= k * k for k in range(4, centre)], axis=0)
    return np.bincount(shell[radius < centre * centre], minlength=centre - 3)


def part_rows(rl):
    first = max(1, 3 * rl // 16)
    return first, (rl - first) // 2, rl - first - (rl - first) // 2


def plan(R, C, turns, portions):
    phases, steps = R.bit_length() - 1, C.bit_length() - 1
    at = {}
    for n, k in enumerate(turns):
        for g in range(2):
            for phase in range(phases):
                at["row", phase, k, g] = 3.0 + 2.2 * n + 3.5 * phase
    for k in turns:
        if k:
            for g in range(2):
                top = k.bit_length()
                ready = [at["row", phases - 1, k, g]]
                ready += [at["col", k | 1 << m, g] for m in range(top, steps)]
                at["col", k, g] = max(ready) + 3.0
    for step in range(steps):
        at["zcol", step] = 4.8 + 4.75 * step
    for phase in range(phases):
        at["zrow", phase] = at["zcol", steps - 1] + 2.5 * (phase + 1)
    for n, k in enumerate(turns[2:]):
        at["send", k] = at["row", 0, turns[n], 1] + 0.1
    at["numbers",] = 3.2
    for n in range(portions):
        at["work", n] = 5.0 + 1.6 * n
    return sorted(at, key=at.get)


def kernel(
    dims,
    bins_hbm, tilt_hbm, part_hbm, table_hbm,
    maps_ref, spectra_ref,
    part_ref, table_ref, bins_ref, tilt_ref, stage_a, stage_b,
    sums_0, sums_1, sums_z, rows_0, rows_1, rows_z, cols_0, cols_1, cols_z, other_map,
    third_ref, numbers, numbers_in, numbers_s, slab_first, slab_second, wide_second,
    bin_first, bin_second, bin_third, weight,
    stats, stats_in, total,
    sent, recv_row, recv_col, recv_zrow, recv_zcol, send_num, recv_num, copy_num,
    send_stat, recv_stat, send_half, recv_half, load_part, load_table, load_bins, load_tilt,
):
    grid, particles, R, C, pitch, bins = dims
    N = R * C
    rl, bl = grid // R, grid // C
    phases, steps = R.bit_length() - 1, C.bit_length() - 1
    half, row, col = lax.axis_index("half"), lax.axis_index("row"), lax.axis_index("col")
    me = row * C + col
    counts = part_rows(rl)
    sums, rows_in, cols_in = (sums_0, sums_1), (rows_0, rows_1), (cols_0, cols_1)

    def peer_id(step):
        peer = (me + step) % N
        return {"row": peer // C, "col": peer % C}

    def flip(index, power):
        return index + (1 - 2 * ((index // power) % 2)) * power

    def power_of(phase, order):
        low, high = 2 ** (phase % phases), 2 ** ((phase + 1) % phases)
        return low + order * (high - low)

    def row_partner(phase, order):
        return {"row": flip(row, power_of(phase, order))}

    def slab_of(index, order):
        slab = row
        for phase in range(phases):
            if (index >> (phases - 1 - phase)) & 1:
                slab = flip(slab, power_of(phase, order))
        return slab

    def col_of(index):
        column = col
        for step in range(steps):
            if (index >> (steps - 1 - step)) & 1:
                column = flip(column, 2 ** step)
        return column

    bins_load = pltpu.make_async_copy(bins_hbm, bins_ref, load_bins)
    tilt_load = pltpu.make_async_copy(tilt_hbm, tilt_ref, load_tilt)
    bins_load.start()
    tilt_load.start()
    table_load = pltpu.make_async_copy(table_hbm, table_ref, load_table)
    table_load.start()
    part_loads = [
        pltpu.make_async_copy(part_hbm.at[p], part_ref.at[p], load_part.at[p])
        for p in range(particles)
    ]
    for copy in part_loads:
        copy.start()

    barrier = pltpu.get_barrier_semaphore()
    for step in range(1, N):
        pl.semaphore_signal(barrier, inc=1, device_id=peer_id(step), device_id_type=MESH)
    pl.semaphore_signal(barrier, inc=1, device_id={"half": 1 - half}, device_id_type=MESH)

    bins_load.wait()
    tilt_load.wait()
    lane = lax.broadcasted_iota(jnp.int32, (1, LANES), 1)
    packed = jnp.zeros((1, LANES), jnp.int32)
    for p in range(particles):
        for i, value in enumerate((bins_ref[p], tilt_ref[p, 0], tilt_ref[p, 1])):
            packed = jnp.where(lane == 3 * p + i, value, packed)
    numbers[0] = packed
    numbers_in[me] = packed

    table_load.wait()
    firsts_, seconds_ = [], []
    for p in range(particles):
        bin_row = bins_ref[p]
        second = table_ref[bin_row, 1].astype(F32)
        for q in range(C):
            slab_second[p, q] = second[q * bl:(q + 1) * bl]
        firsts_.append(table_ref[bin_row, 0])
        seconds_.append(
            jnp.concatenate([slab_second[p, col_of(k)] for k in range(C)], axis=0).astype(BF16)
        )
        third_ref[p * LANES:(p + 1) * LANES, :] = block_diagonal(table_ref[bin_row, 2].T, 2)

    low_lanes = lax.broadcasted_iota(jnp.int32, (grid, LANES), 1) < grid
    for p in range(particles):
        first = firsts_[p]
        mask = wedge_mask(tilt_ref[p, 0], tilt_ref[p, 1], grid, LANES)

        part_loads[p].wait()
        for at in range(grid // 2):
            span = slice(at * LANES, (at + 1) * LANES)
            real, imag = part_ref[p, 0, :, span], part_ref[p, 1, :, span]
            even = jnp.where(low_lanes, real, pltpu.roll(imag, grid, 1)) * mask
            odd = jnp.where(low_lanes, pltpu.roll(real, grid, 1), imag) * mask
            result = dot_nn(first, jnp.concatenate([even, odd], axis=1))
            for o in range(2):
                to = (2 * at + o) * pitch
                stage_a[p, to:to + grid, :] = result[:, o * LANES:(o + 1) * LANES]

    def all_to(src, dst, send, recv):
        return [
            pltpu.make_async_remote_copy(
                src_ref=src.at[0], dst_ref=dst.at[me], send_sem=send, recv_sem=recv,
                device_id=peer_id(step), device_id_type=MESH,
            )
            for step in range(1, N)
        ]

    def whole(dst, send, recv):
        return pltpu.make_async_remote_copy(
            src_ref=dst.at[pl.ds(0, N - 1)], dst_ref=dst.at[pl.ds(0, N - 1)],
            send_sem=send, recv_sem=recv, device_id=peer_id(1), device_id_type=MESH,
        )

    sent_rows = []

    def remote(src, dst, recv, peer, rows):
        copy = pltpu.make_async_remote_copy(
            src_ref=src, dst_ref=dst, send_sem=sent, recv_sem=recv,
            device_id=peer, device_id_type=MESH,
        )
        return copy, rows

    def zcol_copy(step):
        keep = C >> (step + 1)
        span = pl.ds(keep, keep)
        return remote(
            sums_z.at[span], cols_z.at[span], recv_zcol.at[step],
            {"col": flip(col, 2 ** step)}, keep * R * counts[0] * bl,
        )

    def zrow_copy(phase):
        keep = R >> (phase + 1)
        span = pl.ds(keep, keep)
        return remote(
            sums_z.at[0, span], rows_z.at[span], recv_zrow.at[phase],
            row_partner(phase, half), keep * counts[0] * bl,
        )

    def row_copy(phase, k, g):
        keep = R >> (phase + 1)
        span = pl.ds(keep, keep)
        return remote(
            sums[g].at[k, span], rows_in[g].at[k, span], recv_row.at[phase, 2 * k + g],
            row_partner(phase, g), keep * counts[1 + g] * bl,
        )

    def col_copy(k, g):
        step = steps - k.bit_length()
        return remote(
            sums[g].at[k, 0], cols_in[g].at[k], recv_col.at[2 * k + g - 2],
            {"col": flip(col, 2 ** step)}, counts[1 + g] * bl,
        )

    def start(message):
        message[0].start()
        sent_rows.append(message[1])

    firsts_of = [0, R * counts[0], R * (counts[0] + counts[1])]
    within = [0, counts[0], counts[0] + counts[1]]

    def along_second(parts):
        places = [
            (firsts_of[g] + j * counts[g] + i, slab_of(j, order) * rl + within[g] + i)
            for g, order, j0, j1 in parts
            for j in range(j0, j1)
            for i in range(counts[g])
        ]
        for n in range(0, len(places), 2):
            pair = places[n:n + 2]
            for p in range(particles):
                block = jnp.concatenate(
                    [stage_a[p, pl.ds(a, grid, stride=pitch), :] for _, a in pair], axis=1
                ).astype(BF16)
                result = dot_nn(seconds_[p], block).astype(stage_b.dtype)
                for i, (to, _) in enumerate(pair):
                    for k in range(C):
                        stage_b[p, k, to] = result[
                            k * bl:(k + 1) * bl, i * LANES:(i + 1) * LANES
                        ]

    def along_third(parts):
        pieces, places = [], []
        for to, k, g, j0, j1 in parts:
            rows = counts[g] * bl
            low, high = (firsts_of[g] + j * counts[g] for j in (j0, j1))
            pieces.append(jnp.concatenate(
                [
                    stage_b[p, k, low:high].reshape((high - low) * bl, LANES)
                    for p in range(particles)
                ],
                axis=1,
            ))
            places += [(to, k, j, rows) for j in range(j0, j1)]
        result = dot_nn(jnp.concatenate(pieces, axis=0).astype(BF16), third_ref[...])
        at = 0
        for to, k, j, rows in places:
            to[k, j] = result[at:at + rows]
            at += rows

    def row_parts(turn, j0, j1):
        return [(sums[g], k, 1 + g, j0, j1) for k in turn for g in range(2)]

    turns = sorted(
        range(C), key=lambda k: -sum(((k >> i) & 1) << (steps - 1 - i) for i in range(steps))
    )
    along_second([(0, half, 0, R)])
    along_third([(sums_z, k, 0, 0, R) for k in range(C // 2, C)])
    pl.semaphore_wait(barrier, N)
    for copy in all_to(numbers, numbers_in, send_num, recv_num):
        copy.start()
    start(zcol_copy(0))
    along_second([(1 + g, g, R // 2, R) for g in range(2)])
    along_third(row_parts(turns[:1], R // 2, R))
    for g in range(2):
        start(row_copy(0, turns[0], g))
    along_third(row_parts(turns[1:], R // 2, R))
    for g in range(2):
        start(row_copy(0, turns[1], g))
    along_second([(1 + g, g, 0, R // 2) for g in range(2)])
    along_third(row_parts(turns, 0, R // 2) + [(sums_z, k, 0, 0, R) for k in range(C // 2)])

    local = pltpu.make_async_copy(numbers_in, numbers_s, copy_num)
    weight[...] = jnp.zeros_like(weight)
    ones = jnp.ones((grid, LANES), BF16)

    def bin_tables(n, carry):
        first = table_ref[n, 0].astype(F32)
        second = dot_nn(table_ref[n, 1], ones)
        for r in range(R):
            slab_first[0, r] = first[r * rl:(r + 1) * rl]
        for q in range(C):
            wide_second[q] = second[q * bl:(q + 1) * bl]
        bin_first[n] = slab_first[0, row]
        bin_second[n] = wide_second[col]
        across = table_ref[n, 2].T
        bin_third[n] = jnp.concatenate([across, across], axis=1)
        return carry

    lax.fori_loop(0, bins, bin_tables, 0, unroll=4)

    together = 2
    first_wave = lax.broadcasted_iota(jnp.int32, (grid, LANES), 0) - grid // 2
    third_wave = lax.broadcasted_iota(jnp.int32, (grid, LANES), 1) % grid - grid // 2
    same_side = first_wave * third_wave >= 0
    first_size, third_size = jnp.abs(first_wave), 16 * jnp.abs(third_wave)
    low_rows = lax.broadcasted_iota(jnp.int32, (rl, LANES), 1) < grid
    low_seconds = lax.broadcasted_iota(jnp.int32, (bl, LANES), 1) < grid

    def add_weight(step, carry):
        members = [(step * together + n, p) for n in range(together) for p in range(particles)]
        blocks, thirds = [], []
        for i in range(0, len(members), 2):
            numbers_of = [
                [numbers_s[n, 0, 3 * p + v] for v in range(3)] for n, p in members[i:i + 2]
            ]
            limit = jnp.where(
                same_side,
                jnp.where(low_lanes, numbers_of[0][1], numbers_of[1][1]),
                jnp.where(low_lanes, numbers_of[0][2], numbers_of[1][2]),
            )
            mask = jnp.where(third_size <= limit * first_size, 1.0, 0.0).astype(BF16)
            along = [dot_nn(bin_first[value[0]].astype(BF16), mask) for value in numbers_of]
            first = jnp.where(low_rows, along[0], along[1]).astype(BF16).astype(F32)
            second = jnp.where(
                low_seconds, bin_second[numbers_of[0][0]], bin_second[numbers_of[1][0]]
            )
            blocks.append(
                jnp.concatenate([first[a:a + 1] * second for a in range(rl)], axis=0).astype(BF16)
            )
            thirds += [bin_third[value[0]] for value in numbers_of]
        weight[...] += dot_nn(jnp.concatenate(blocks, axis=1), jnp.concatenate(thirds, axis=0))
        return carry

    groups = N // together
    portions = 8
    done = set()
    worked = [0]

    def work():
        n = worked[0]
        worked[0] = n + 1
        if n == 0:
            local.wait()
        low, high = groups * n // portions, groups * (n + 1) // portions
        if high > low:
            lax.fori_loop(low, high, add_weight, 0)

    def col_ready(k, g):
        top = k.bit_length()
        return all(("row", phases - 1, k, g) in done and ("col", k | 1 << m, g) in done for m in range(top, steps)) and ("row", phases - 1, k, g) in done

    def maybe_col(k, g):
        if k and col_ready(k, g) and ("sentcol", k, g) not in done:
            done.add(("sentcol", k, g))
            start(col_copy(k, g))

    def take(event):
        kind = event[0]
        if kind == "work":
            work()
            return
        if kind == "send":
            for g in range(2):
                start(row_copy(0, event[1], g))
            return
        if kind == "numbers":
            whole(numbers_in, send_num, recv_num).wait_recv()
            local.start()
            return
        if kind == "zcol":
            zcol_copy(event[1])[0].wait_recv()
        elif kind == "zrow":
            zrow_copy(event[1])[0].wait_recv()
        elif kind == "row":
            row_copy(*event[1:])[0].wait_recv()
        else:
            col_copy(*event[1:])[0].wait_recv()
        done.add(event)
        if kind == "zcol":
            step = event[1]
            keep = C >> (step + 1)
            sums_z[:keep] = sums_z[:keep] + cols_z[keep:2 * keep]
            start(zcol_copy(step + 1) if step + 1 < steps else zrow_copy(0))
        elif kind == "zrow":
            phase = event[1]
            keep = R >> (phase + 1)
            sums_z[0, :keep] = sums_z[0, :keep] + rows_z[keep:2 * keep]
            if phase + 1 < phases:
                start(zrow_copy(phase + 1))
        elif kind == "row":
            _, phase, k, g = event
            keep = R >> (phase + 1)
            sums[g][k, :keep] = sums[g][k, :keep] + rows_in[g][k, keep:2 * keep]
            if phase + 1 < phases:
                start(row_copy(phase + 1, k, g))
            else:
                maybe_col(k, g)
        else:
            _, k, g = event
            into = k - (1 << k.bit_length() - 1)
            sums[g][into, 0] = sums[g][into, 0] + cols_in[g][k]
            maybe_col(into, g)

    for event in plan(R, C, turns, portions):
        take(event)

    block = jnp.concatenate([sums_z[0, 0], sums_0[0, 0], sums_1[0, 0]], axis=0)
    weight[...] = block / (weight[...] + 1.0)
    low = lax.broadcasted_iota(jnp.int32, (rl, LANES), 1) < grid
    for pair in range(bl // 2):
        span = slice(pair * LANES, (pair + 1) * LANES)
        even, odd = (weight[pl.ds(2 * pair + i, rl, stride=bl), :] for i in range(2))
        maps_ref[0, 0, :, span] = jnp.where(low, even, pltpu.roll(odd, grid, 1))
        maps_ref[0, 1, :, span] = jnp.where(low, pltpu.roll(even, grid, 1), odd)

    half_copy = pltpu.make_async_remote_copy(
        src_ref=maps_ref.at[0], dst_ref=other_map, send_sem=send_half, recv_sem=recv_half,
        device_id={"half": 1 - half}, device_id_type=MESH,
    )
    half_copy.start()
    everything = stage_a.at[0, pl.ds(0, sum(sent_rows))]
    pltpu.make_async_remote_copy(
        src_ref=everything, dst_ref=everything, send_sem=sent, recv_sem=recv_half,
        device_id={"half": 1 - half}, device_id_type=MESH,
    ).wait_send()
    whole(numbers_in, send_num, recv_num).wait_send()

    centre = grid // 2
    shells = centre - 3
    tile_rows = lax.broadcasted_iota(jnp.int32, (rl, LANES), 0)
    tile_lanes = lax.broadcasted_iota(jnp.int32, (rl, LANES), 1)
    wave_first = row * rl + tile_rows - centre
    wave_third = tile_lanes % grid - centre
    fixed = wave_first * wave_first + wave_third * wave_third
    radius = []
    for pair in range(bl // 2):
        wave_second = col * bl + 2 * pair + tile_lanes // grid - centre
        radius.append(fixed + wave_second * wave_second)
    stats[...] = jnp.zeros_like(stats)

    def shell_sums(rows_at, values):
        for s in range(shells):
            least = (s + 3) * (s + 3) if s else 0
            beyond = (s + 4) * (s + 4)
            parts = [jnp.zeros((rl, LANES), F32) for _ in values]
            for pair, r2 in enumerate(radius):
                inside = (r2 >= least) & (r2 < beyond)
                parts = [
                    part + jnp.where(inside, value[pair], 0.0)
                    for part, value in zip(parts, values)
                ]
            for at, part in zip(rows_at, parts):
                stats[pl.ds(at + s, 1), :] = jnp.sum(part, axis=0, keepdims=True)

    def tiles(ref, c):
        return [ref[c, :, pair * LANES:(pair + 1) * LANES] for pair in range(bl // 2)]

    mine = [tiles(maps_ref.at[0], c) for c in range(2)]
    shell_sums([32 + 32 * half], [[x * x + y * y for x, y in zip(*mine)]])
    half_copy.wait()
    theirs = [tiles(other_map, c) for c in range(2)]
    mine = [tiles(maps_ref.at[0], c) for c in range(2)]
    shell_sums(
        [0, 64 - 32 * half],
        [
            [x * u + y * v for x, y, u, v in zip(*mine, *theirs)],
            [u * u + v * v for u, v in zip(*theirs)],
        ],
    )
    mine = jnp.sum(stats[...].T, axis=0, keepdims=True)
    total[0] = mine
    stats_in[me] = mine
    for copy in all_to(total, stats_in, send_stat, recv_stat):
        copy.start()
    whole(stats_in, send_stat, recv_stat).wait()
    spectra = stats_in[0]
    for n in range(1, N):
        spectra = spectra + stats_in[n]
    spectra_ref[...] = spectra


def finish(shells, maps_in_ref, spectra_ref, counts_ref, maps_ref, power_ref, corr_ref):
    maps_ref[...] = maps_in_ref[...]
    spectra = spectra_ref[...]
    cross = spectra[:, 0:shells]
    power_first = spectra[:, 32:32 + shells]
    power_second = spectra[:, 64:64 + shells]
    power_ref[0:1, :] = power_first / counts_ref[...]
    power_ref[1:2, :] = power_second / counts_ref[...]
    corr_ref[...] = cross / jnp.sqrt(power_first * power_second + 1e-6)


def solution(mesh):
    R, C = mesh.shape["row"], mesh.shape["col"]
    N = R * C

    def local(particles, orient_bin, tilt_slope, interp_table):
        count, _, grid, plane = particles.shape
        rl, cl, bl = grid // R, plane // C, grid // C
        shells = grid // 2 - 3
        phases = R.bit_length() - 1
        pitch = grid + 8
        bins = interp_table.shape[0]
        steps = C.bit_length() - 1
        nz, n0, n1 = part_rows(rl)
        counts = jnp.asarray(shell_counts(grid)[None], F32)
        vmem, hbm = pl.BlockSpec(memory_space=pltpu.VMEM), pl.BlockSpec(memory_space=pltpu.HBM)
        dma = pltpu.SemaphoreType.DMA
        maps, spectra = pl.pallas_call(
            functools.partial(kernel, (grid, count, R, C, pitch, bins)),
            out_shape=(
                pltpu.VMEM((1, 2, rl, cl), F32),
                pltpu.VMEM((1, LANES), F32),
            ),
            in_specs=[hbm, hbm, hbm, hbm],
            out_specs=(vmem, vmem),
            scratch_shapes=[
                pltpu.VMEM(particles.shape, particles.dtype),
                pltpu.VMEM(interp_table.shape, interp_table.dtype),
                pltpu.SMEM(orient_bin.shape, jnp.int32),
                pltpu.SMEM(tilt_slope.shape, jnp.int32),
                pltpu.VMEM((count, grid * pitch, LANES), F32),
                pltpu.VMEM((count, C, grid, bl, LANES), F32 if bl % 16 else BF16),
                pltpu.VMEM((C, R, n0 * bl, LANES), F32),
                pltpu.VMEM((C, R, n1 * bl, LANES), F32),
                pltpu.VMEM((C, R, nz * bl, LANES), F32),
                pltpu.VMEM((C, R, n0 * bl, LANES), F32),
                pltpu.VMEM((C, R, n1 * bl, LANES), F32),
                pltpu.VMEM((R, nz * bl, LANES), F32),
                pltpu.VMEM((C, n0 * bl, LANES), F32),
                pltpu.VMEM((C, n1 * bl, LANES), F32),
                pltpu.VMEM((C, R, nz * bl, LANES), F32),
                pltpu.VMEM((2, rl, cl), F32),
                pltpu.VMEM((count * LANES, LANES), BF16),
                pltpu.VMEM((1, 1, LANES), jnp.int32),
                pltpu.VMEM((N, 1, LANES), jnp.int32),
                pltpu.SMEM((N, 1, LANES), jnp.int32),
                pltpu.VMEM((count, R, rl, grid), F32),
                pltpu.VMEM((count, C, bl, grid), F32),
                pltpu.VMEM((C, bl, LANES), F32),
                pltpu.VMEM((bins, rl, grid), F32),
                pltpu.VMEM((bins, bl, LANES), F32),
                pltpu.VMEM((bins, grid, LANES), BF16),
                pltpu.VMEM((rl * bl, LANES), F32),
                pltpu.VMEM((LANES, LANES), F32),
                pltpu.VMEM((N, 1, LANES), F32),
                pltpu.VMEM((1, 1, LANES), F32),
                dma, dma((phases, 2 * C)), dma((2 * C - 2,)),
                dma((phases,)), dma((steps,)),
                dma, dma, dma,
                dma, dma,
                dma, dma, dma((count,)), dma, dma, dma,
            ],
            compiler_params=pltpu.CompilerParams(
                collective_id=0, has_side_effects=True, vmem_limit_bytes=VMEM_LIMIT
            ),
        )(orient_bin, tilt_slope, particles, interp_table)
        return pl.pallas_call(
            functools.partial(finish, shells),
            out_shape=(
                jax.ShapeDtypeStruct((1, 2, rl, cl), F32),
                jax.ShapeDtypeStruct((2, shells), F32),
                jax.ShapeDtypeStruct((1, shells), F32),
            ),
            in_specs=[vmem, vmem, vmem],
            out_specs=(vmem, vmem, vmem),
            compiler_params=pltpu.CompilerParams(vmem_limit_bytes=FINISH_LIMIT),
        )(maps, spectra, counts)

    placed = (
        P(("half", "row", "col"), None, None, None),
        P(("half", "row", "col")),
        P(("half", "row", "col"), None),
        P(),
    )
    return jax.shard_map(
        local,
        mesh=mesh,
        in_specs=placed,
        out_specs=(P("half", None, "row", "col"), P(), P("half", None)),
        check_vma=False,
    )
```

```python
import functools

import jax
import jax.numpy as jnp
import numpy as np
from jax import lax
from jax.experimental import pallas as pl
from jax.experimental.pallas import tpu as pltpu
from jax.sharding import PartitionSpec as P

F32 = jnp.float32
BF16 = jnp.bfloat16
LANES = 128
VMEM_LIMIT = 60 * 1024 * 1024
FINISH_LIMIT = 4 * 1024 * 1024
MESH = pl.DeviceIdType.MESH


def dot_nt(left, right):
    return lax.dot_general(left, right, (((1,), (1,)), ((), ())), preferred_element_type=F32)


def dot_nn(left, right):
    return lax.dot_general(left, right, (((1,), (0,)), ((), ())), preferred_element_type=F32)


def block_diagonal(block, copies):
    zero = jnp.zeros_like(block)
    rows = [
        jnp.concatenate([block if i == j else zero for j in range(copies)], axis=1)
        for i in range(copies)
    ]
    return jnp.concatenate(rows, axis=0)


def wedge_mask(limit_same, limit_other, grid, lanes):
    centre = grid // 2
    first = lax.broadcasted_iota(jnp.int32, (grid, lanes), 0) - centre
    third = lax.broadcasted_iota(jnp.int32, (grid, lanes), 1) % grid - centre
    limit = jnp.where(first * third >= 0, limit_same, limit_other)
    inside = 16 * jnp.abs(third) <= limit * jnp.abs(first)
    return jnp.where(inside, 1.0, 0.0).astype(BF16)


def shell_counts(grid):
    centre = grid // 2
    wave = np.arange(grid) - centre
    square = wave * wave
    radius = square[:, None, None] + square[None, :, None] + square[None, None, :]
    shell = np.sum([radius >= k * k for k in range(4, centre)], axis=0)
    return np.bincount(shell[radius < centre * centre], minlength=centre - 3)


def part_rows(rl):
    first = max(1, 3 * rl // 16)
    return first, (rl - first) // 2, rl - first - (rl - first) // 2


def plan(R, C, turns, portions):
    phases, steps = R.bit_length() - 1, C.bit_length() - 1
    at = {}
    for n, k in enumerate(turns):
        for g in range(2):
            for phase in range(phases):
                at["row", phase, k, g] = 3.0 + 2.2 * n + 3.5 * phase
    for k in turns:
        if k:
            for g in range(2):
                top = k.bit_length()
                ready = [at["row", phases - 1, k, g]]
                ready += [at["col", k | 1 << m, g] for m in range(top, steps)]
                at["col", k, g] = max(ready) + 3.0
    for step in range(steps):
        at["zcol", step] = 4.8 + 4.75 * step
    for phase in range(phases):
        at["zrow", phase] = at["zcol", steps - 1] + 2.5 * (phase + 1)
    for n, k in enumerate(turns[2:]):
        at["send", k] = at["row", 0, turns[n], 1] + 0.1
    at["numbers",] = 3.2
    for n in range(portions):
        at["work", n] = 5.0 + 1.1 * n
    return sorted(at, key=at.get)


def kernel(
    dims,
    bins_hbm, tilt_hbm, part_hbm, table_hbm,
    maps_ref, spectra_ref,
    part_ref, table_ref, bins_ref, tilt_ref, stage_a, stage_b,
    sums_0, sums_1, sums_z, rows_0, rows_1, rows_z, cols_0, cols_1, cols_z, other_map,
    third_ref, numbers, numbers_in, numbers_s, slab_first, slab_second, wide_second,
    bin_first, bin_second, bin_third, weight,
    inside, stats, stats_in, total,
    sent, recv_row, recv_col, recv_zrow, recv_zcol, recv_num, copy_num,
    recv_stat, recv_half, load_part, load_table, load_bins, load_tilt,
):
    grid, particles, R, C, pitch, bins = dims
    N = R * C
    rl, bl = grid // R, grid // C
    phases, steps = R.bit_length() - 1, C.bit_length() - 1
    half, row, col = lax.axis_index("half"), lax.axis_index("row"), lax.axis_index("col")
    me = row * C + col
    counts = part_rows(rl)
    sums, rows_in, cols_in = (sums_0, sums_1), (rows_0, rows_1), (cols_0, cols_1)

    def peer_id(step):
        peer = (me + step) % N
        return {"row": peer // C, "col": peer % C}

    def flip(index, power):
        return index + (1 - 2 * ((index // power) % 2)) * power

    def power_of(phase, order):
        low, high = 2 ** (phase % phases), 2 ** ((phase + 1) % phases)
        return low + order * (high - low)

    def row_partner(phase, order):
        return {"row": flip(row, power_of(phase, order))}

    def slab_of(index, order):
        slab = row
        for phase in range(phases):
            if (index >> (phases - 1 - phase)) & 1:
                slab = flip(slab, power_of(phase, order))
        return slab

    def col_of(index):
        column = col
        for step in range(steps):
            if (index >> (steps - 1 - step)) & 1:
                column = flip(column, 2 ** step)
        return column

    bins_load = pltpu.make_async_copy(bins_hbm, bins_ref, load_bins)
    tilt_load = pltpu.make_async_copy(tilt_hbm, tilt_ref, load_tilt)
    bins_load.start()
    tilt_load.start()
    table_load = pltpu.make_async_copy(table_hbm, table_ref, load_table)
    table_load.start()
    part_loads = [
        pltpu.make_async_copy(part_hbm.at[p], part_ref.at[p], load_part.at[p])
        for p in range(particles)
    ]
    for copy in part_loads:
        copy.start()

    barrier = pltpu.get_barrier_semaphore()
    for step in range(1, N):
        pl.semaphore_signal(barrier, inc=1, device_id=peer_id(step), device_id_type=MESH)
    pl.semaphore_signal(barrier, inc=1, device_id={"half": 1 - half}, device_id_type=MESH)

    bins_load.wait()
    tilt_load.wait()
    lane = lax.broadcasted_iota(jnp.int32, (1, LANES), 1)
    packed = jnp.zeros((1, LANES), jnp.int32)
    for p in range(particles):
        for i, value in enumerate((bins_ref[p], tilt_ref[p, 0], tilt_ref[p, 1])):
            packed = jnp.where(lane == 3 * p + i, value, packed)
    numbers[0] = packed
    numbers_in[me] = packed

    table_load.wait()
    firsts_, seconds_ = [], []
    for p in range(particles):
        bin_row = bins_ref[p]
        second = table_ref[bin_row, 1].astype(F32)
        for q in range(C):
            slab_second[p, q] = second[q * bl:(q + 1) * bl]
        firsts_.append(table_ref[bin_row, 0])
        seconds_.append(
            jnp.concatenate([slab_second[p, col_of(k)] for k in range(C)], axis=0).astype(BF16)
        )
        third_ref[p * LANES:(p + 1) * LANES, :] = block_diagonal(table_ref[bin_row, 2].T, 2)

    low_lanes = lax.broadcasted_iota(jnp.int32, (grid, LANES), 1) < grid
    for p in range(particles):
        first = firsts_[p]
        mask = wedge_mask(tilt_ref[p, 0], tilt_ref[p, 1], grid, LANES)

        part_loads[p].wait()
        for at in range(grid // 2):
            span = slice(at * LANES, (at + 1) * LANES)
            real, imag = part_ref[p, 0, :, span], part_ref[p, 1, :, span]
            even = jnp.where(low_lanes, real, pltpu.roll(imag, grid, 1)) * mask
            odd = jnp.where(low_lanes, pltpu.roll(real, grid, 1), imag) * mask
            result = dot_nn(first, jnp.concatenate([even, odd], axis=1))
            for o in range(2):
                to = (2 * at + o) * pitch
                stage_a[p, to:to + grid, :] = result[:, o * LANES:(o + 1) * LANES]

    def all_to(src, dst, recv):
        return [
            pltpu.make_async_remote_copy(
                src_ref=src.at[0], dst_ref=dst.at[me], send_sem=sent, recv_sem=recv,
                device_id=peer_id(step), device_id_type=MESH,
            )
            for step in range(1, N)
        ]

    def whole(dst, recv):
        return pltpu.make_async_remote_copy(
            src_ref=dst.at[pl.ds(0, N - 1)], dst_ref=dst.at[pl.ds(0, N - 1)],
            send_sem=sent, recv_sem=recv, device_id=peer_id(1), device_id_type=MESH,
        )

    sent_rows = []

    def remote(src, dst, recv, peer, rows):
        copy = pltpu.make_async_remote_copy(
            src_ref=src, dst_ref=dst, send_sem=sent, recv_sem=recv,
            device_id=peer, device_id_type=MESH,
        )
        return copy, rows

    def zcol_copy(step):
        keep = C >> (step + 1)
        span = pl.ds(keep, keep)
        return remote(
            sums_z.at[span], cols_z.at[span], recv_zcol.at[step],
            {"col": flip(col, 2 ** step)}, keep * R * counts[0] * bl,
        )

    def zrow_copy(phase):
        keep = R >> (phase + 1)
        span = pl.ds(keep, keep)
        return remote(
            sums_z.at[0, span], rows_z.at[span], recv_zrow.at[phase],
            row_partner(phase, half), keep * counts[0] * bl,
        )

    def row_copy(phase, k, g):
        keep = R >> (phase + 1)
        span = pl.ds(keep, keep)
        return remote(
            sums[g].at[k, span], rows_in[g].at[k, span], recv_row.at[phase, 2 * k + g],
            row_partner(phase, g), keep * counts[1 + g] * bl,
        )

    def col_copy(k, g):
        step = steps - k.bit_length()
        return remote(
            sums[g].at[k, 0], cols_in[g].at[k], recv_col.at[2 * k + g - 2],
            {"col": flip(col, 2 ** step)}, counts[1 + g] * bl,
        )

    def start(message):
        message[0].start()
        sent_rows.append(message[1])

    firsts_of = [0, R * counts[0], R * (counts[0] + counts[1])]
    within = [0, counts[0], counts[0] + counts[1]]

    def along_second(parts):
        places = [
            (firsts_of[g] + j * counts[g] + i, slab_of(j, order) * rl + within[g] + i)
            for g, order, j0, j1 in parts
            for j in range(j0, j1)
            for i in range(counts[g])
        ]
        for n in range(0, len(places), 2):
            pair = places[n:n + 2]
            for p in range(particles):
                block = jnp.concatenate(
                    [stage_a[p, pl.ds(a, grid, stride=pitch), :] for _, a in pair], axis=1
                ).astype(BF16)
                result = dot_nn(seconds_[p], block).astype(stage_b.dtype)
                for i, (to, _) in enumerate(pair):
                    for k in range(C):
                        stage_b[p, k, to] = result[
                            k * bl:(k + 1) * bl, i * LANES:(i + 1) * LANES
                        ]

    def along_third(parts):
        pieces, places = [], []
        for to, k, g, j0, j1 in parts:
            rows = counts[g] * bl
            low, high = (firsts_of[g] + j * counts[g] for j in (j0, j1))
            pieces.append(jnp.concatenate(
                [
                    stage_b[p, k, low:high].reshape((high - low) * bl, LANES)
                    for p in range(particles)
                ],
                axis=1,
            ))
            places += [(to, k, j, rows) for j in range(j0, j1)]
        result = dot_nn(jnp.concatenate(pieces, axis=0).astype(BF16), third_ref[...])
        at = 0
        for to, k, j, rows in places:
            to[k, j] = result[at:at + rows]
            at += rows

    def row_parts(turn, j0, j1):
        return [(sums[g], k, 1 + g, j0, j1) for k in turn for g in range(2)]

    turns = sorted(
        range(C), key=lambda k: -sum(((k >> i) & 1) << (steps - 1 - i) for i in range(steps))
    )
    along_second([(0, half, 0, R)])
    along_third([(sums_z, k, 0, 0, R) for k in range(C // 2, C)])
    pl.semaphore_wait(barrier, N)
    for copy in all_to(numbers, numbers_in, recv_num):
        copy.start()
    start(zcol_copy(0))
    along_second([(1 + g, g, R // 2, R) for g in range(2)])
    along_third(row_parts(turns[:1], R // 2, R))
    for g in range(2):
        start(row_copy(0, turns[0], g))
    along_third(row_parts(turns[1:], R // 2, R))
    for g in range(2):
        start(row_copy(0, turns[1], g))
    along_second([(1 + g, g, 0, R // 2) for g in range(2)])
    along_third(row_parts(turns, 0, R // 2) + [(sums_z, k, 0, 0, R) for k in range(C // 2)])

    local = pltpu.make_async_copy(numbers_in, numbers_s, copy_num)
    weight[...] = jnp.zeros_like(weight)
    ones = jnp.ones((grid, LANES), BF16)

    def bin_tables(n, carry):
        first = table_ref[n, 0].astype(F32)
        second = dot_nn(table_ref[n, 1], ones)
        for r in range(R):
            slab_first[0, r] = first[r * rl:(r + 1) * rl]
        for q in range(C):
            wide_second[q] = second[q * bl:(q + 1) * bl]
        bin_first[n] = slab_first[0, row]
        bin_second[n] = wide_second[col]
        across = table_ref[n, 2].T
        bin_third[n] = jnp.concatenate([across, across], axis=1)
        return carry

    lax.fori_loop(0, bins, bin_tables, 0, unroll=4)

    together = 2
    first_wave = lax.broadcasted_iota(jnp.int32, (grid, LANES), 0) - grid // 2
    third_wave = lax.broadcasted_iota(jnp.int32, (grid, LANES), 1) % grid - grid // 2
    same_side = first_wave * third_wave >= 0
    first_size, third_size = jnp.abs(first_wave), 16 * jnp.abs(third_wave)
    low_rows = lax.broadcasted_iota(jnp.int32, (rl, LANES), 1) < grid
    low_seconds = lax.broadcasted_iota(jnp.int32, (bl, LANES), 1) < grid

    def add_weight(step, carry):
        members = [(step * together + n, p) for n in range(together) for p in range(particles)]
        blocks, thirds = [], []
        for i in range(0, len(members), 2):
            numbers_of = [
                [numbers_s[n, 0, 3 * p + v] for v in range(3)] for n, p in members[i:i + 2]
            ]
            limit = jnp.where(
                same_side,
                jnp.where(low_lanes, numbers_of[0][1], numbers_of[1][1]),
                jnp.where(low_lanes, numbers_of[0][2], numbers_of[1][2]),
            )
            mask = jnp.where(third_size <= limit * first_size, 1.0, 0.0).astype(BF16)
            along = [dot_nn(bin_first[value[0]].astype(BF16), mask) for value in numbers_of]
            first = jnp.where(low_rows, along[0], along[1]).astype(BF16).astype(F32)
            second = jnp.where(
                low_seconds, bin_second[numbers_of[0][0]], bin_second[numbers_of[1][0]]
            )
            blocks.append(
                jnp.concatenate([first[a:a + 1] * second for a in range(rl)], axis=0).astype(BF16)
            )
            thirds += [bin_third[value[0]] for value in numbers_of]
        weight[...] += dot_nn(jnp.concatenate(blocks, axis=1), jnp.concatenate(thirds, axis=0))
        return carry

    centre = grid // 2
    shells = centre - 3
    tile_rows = lax.broadcasted_iota(jnp.int32, (rl, LANES), 0)
    tile_lanes = lax.broadcasted_iota(jnp.int32, (rl, LANES), 1)
    wave_first = row * rl + tile_rows - centre
    wave_third = tile_lanes % grid - centre
    fixed = wave_first * wave_first + wave_third * wave_third
    radius = []
    for pair in range(bl // 2):
        wave_second = col * bl + 2 * pair + tile_lanes // grid - centre
        radius.append(fixed + wave_second * wave_second)
    for s in range(shells):
        least = (s + 3) * (s + 3) if s else 0
        beyond = (s + 4) * (s + 4)
        for pair, r2 in enumerate(radius):
            inside[s, pair] = jnp.where((r2 >= least) & (r2 < beyond), 1.0, 0.0)

    groups = N // together
    portions = 8
    done = set()
    worked = [0]

    def work():
        n = worked[0]
        worked[0] = n + 1
        if n == 0:
            local.wait()
        low, high = groups * n // portions, groups * (n + 1) // portions
        if high > low:
            lax.fori_loop(low, high, add_weight, 0)

    def col_ready(k, g):
        top = k.bit_length()
        return all(("row", phases - 1, k, g) in done and ("col", k | 1 << m, g) in done for m in range(top, steps)) and ("row", phases - 1, k, g) in done

    def maybe_col(k, g):
        if k and col_ready(k, g) and ("sentcol", k, g) not in done:
            done.add(("sentcol", k, g))
            start(col_copy(k, g))

    def take(event):
        kind = event[0]
        if kind == "work":
            work()
            return
        if kind == "send":
            for g in range(2):
                start(row_copy(0, event[1], g))
            return
        if kind == "numbers":
            whole(numbers_in, recv_num).wait_recv()
            local.start()
            return
        if kind == "zcol":
            zcol_copy(event[1])[0].wait_recv()
        elif kind == "zrow":
            zrow_copy(event[1])[0].wait_recv()
        elif kind == "row":
            row_copy(*event[1:])[0].wait_recv()
        else:
            col_copy(*event[1:])[0].wait_recv()
        done.add(event)
        if kind == "zcol":
            step = event[1]
            keep = C >> (step + 1)
            sums_z[:keep] = sums_z[:keep] + cols_z[keep:2 * keep]
            start(zcol_copy(step + 1) if step + 1 < steps else zrow_copy(0))
        elif kind == "zrow":
            phase = event[1]
            keep = R >> (phase + 1)
            sums_z[0, :keep] = sums_z[0, :keep] + rows_z[keep:2 * keep]
            if phase + 1 < phases:
                start(zrow_copy(phase + 1))
        elif kind == "row":
            _, phase, k, g = event
            keep = R >> (phase + 1)
            sums[g][k, :keep] = sums[g][k, :keep] + rows_in[g][k, keep:2 * keep]
            if phase + 1 < phases:
                start(row_copy(phase + 1, k, g))
            else:
                maybe_col(k, g)
        else:
            _, k, g = event
            into = k - (1 << k.bit_length() - 1)
            sums[g][into, 0] = sums[g][into, 0] + cols_in[g][k]
            maybe_col(into, g)

    for event in plan(R, C, turns, portions):
        take(event)

    block = jnp.concatenate([sums_z[0, 0], sums_0[0, 0], sums_1[0, 0]], axis=0)
    weight[...] = block / (weight[...] + 1.0)
    low = lax.broadcasted_iota(jnp.int32, (rl, LANES), 1) < grid
    for pair in range(bl // 2):
        span = slice(pair * LANES, (pair + 1) * LANES)
        even, odd = (weight[pl.ds(2 * pair + i, rl, stride=bl), :] for i in range(2))
        maps_ref[0, 0, :, span] = jnp.where(low, even, pltpu.roll(odd, grid, 1))
        maps_ref[0, 1, :, span] = jnp.where(low, pltpu.roll(even, grid, 1), odd)

    half_copy = pltpu.make_async_remote_copy(
        src_ref=maps_ref.at[0], dst_ref=other_map, send_sem=sent, recv_sem=recv_half,
        device_id={"half": 1 - half}, device_id_type=MESH,
    )
    half_copy.start()
    stats[...] = jnp.zeros_like(stats)

    def shell_sums(rows_at, values):
        for s in range(shells):
            parts = [jnp.zeros((rl, LANES), F32) for _ in values]
            for pair in range(bl // 2):
                mask = inside[s, pair]
                parts = [part + mask * value[pair] for part, value in zip(parts, values)]
            for at, part in zip(rows_at, parts):
                stats[pl.ds(at + s, 1), :] = jnp.sum(part, axis=0, keepdims=True)

    def tiles(ref, c):
        return [ref[c, :, pair * LANES:(pair + 1) * LANES] for pair in range(bl // 2)]

    mine = [tiles(maps_ref.at[0], c) for c in range(2)]
    shell_sums([32 + 32 * half], [[x * x + y * y for x, y in zip(*mine)]])
    half_copy.wait_recv()
    theirs = [tiles(other_map, c) for c in range(2)]
    mine = [tiles(maps_ref.at[0], c) for c in range(2)]
    shell_sums(
        [0, 64 - 32 * half],
        [
            [x * u + y * v for x, y, u, v in zip(*mine, *theirs)],
            [u * u + v * v for u, v in zip(*theirs)],
        ],
    )
    mine = jnp.sum(stats[...].T, axis=0, keepdims=True)
    total[0] = mine
    stats_in[me] = mine
    for copy in all_to(total, stats_in, recv_stat):
        copy.start()
    whole(stats_in, recv_stat).wait_recv()
    spectra = stats_in[0]
    for n in range(1, N):
        spectra = spectra + stats_in[n]
    spectra_ref[...] = spectra
    rows = sum(sent_rows) + 2 * (N - 1) + 2 * rl * bl * grid // LANES
    everything = stage_a.at[0, pl.ds(0, rows)]
    pltpu.make_async_remote_copy(
        src_ref=everything, dst_ref=everything, send_sem=sent, recv_sem=recv_half,
        device_id={"half": 1 - half}, device_id_type=MESH,
    ).wait_send()


def finish(shells, maps_in, spectra_ref, counts_ref, maps, power, corr, power_ref, corr_ref, done):
    maps_out = pltpu.make_async_copy(maps_in, maps, done.at[0])
    maps_out.start()
    spectra = spectra_ref[...]
    cross = spectra[:, 0:shells]
    power_first = spectra[:, 32:32 + shells]
    power_second = spectra[:, 64:64 + shells]
    power_ref[0:1, :] = power_first / counts_ref[...]
    power_ref[1:2, :] = power_second / counts_ref[...]
    corr_ref[...] = cross / jnp.sqrt(power_first * power_second + 1e-6)
    small = [
        pltpu.make_async_copy(power_ref, power, done.at[1]),
        pltpu.make_async_copy(corr_ref, corr, done.at[2]),
    ]
    for copy in small:
        copy.start()
    for copy in [maps_out] + small:
        copy.wait()


def solution(mesh):
    R, C = mesh.shape["row"], mesh.shape["col"]
    N = R * C

    def local(particles, orient_bin, tilt_slope, interp_table):
        count, _, grid, plane = particles.shape
        rl, cl, bl = grid // R, plane // C, grid // C
        shells = grid // 2 - 3
        phases = R.bit_length() - 1
        pitch = grid + 8
        bins = interp_table.shape[0]
        steps = C.bit_length() - 1
        nz, n0, n1 = part_rows(rl)
        counts = jnp.asarray(shell_counts(grid)[None], F32)
        vmem, hbm = pl.BlockSpec(memory_space=pltpu.VMEM), pl.BlockSpec(memory_space=pltpu.HBM)
        dma = pltpu.SemaphoreType.DMA
        maps, spectra = pl.pallas_call(
            functools.partial(kernel, (grid, count, R, C, pitch, bins)),
            out_shape=(
                pltpu.VMEM((1, 2, rl, cl), F32),
                pltpu.VMEM((1, LANES), F32),
            ),
            in_specs=[hbm, hbm, hbm, hbm],
            out_specs=(vmem, vmem),
            scratch_shapes=[
                pltpu.VMEM(particles.shape, particles.dtype),
                pltpu.VMEM(interp_table.shape, interp_table.dtype),
                pltpu.SMEM(orient_bin.shape, jnp.int32),
                pltpu.SMEM(tilt_slope.shape, jnp.int32),
                pltpu.VMEM((count, grid * pitch, LANES), F32),
                pltpu.VMEM((count, C, grid, bl, LANES), F32 if bl % 16 else BF16),
                pltpu.VMEM((C, R, n0 * bl, LANES), F32),
                pltpu.VMEM((C, R, n1 * bl, LANES), F32),
                pltpu.VMEM((C, R, nz * bl, LANES), F32),
                pltpu.VMEM((C, R, n0 * bl, LANES), F32),
                pltpu.VMEM((C, R, n1 * bl, LANES), F32),
                pltpu.VMEM((R, nz * bl, LANES), F32),
                pltpu.VMEM((C, n0 * bl, LANES), F32),
                pltpu.VMEM((C, n1 * bl, LANES), F32),
                pltpu.VMEM((C, R, nz * bl, LANES), F32),
                pltpu.VMEM((2, rl, cl), F32),
                pltpu.VMEM((count * LANES, LANES), BF16),
                pltpu.VMEM((1, 1, LANES), jnp.int32),
                pltpu.VMEM((N, 1, LANES), jnp.int32),
                pltpu.SMEM((N, 1, LANES), jnp.int32),
                pltpu.VMEM((count, R, rl, grid), F32),
                pltpu.VMEM((count, C, bl, grid), F32),
                pltpu.VMEM((C, bl, LANES), F32),
                pltpu.VMEM((bins, rl, grid), F32),
                pltpu.VMEM((bins, bl, LANES), F32),
                pltpu.VMEM((bins, grid, LANES), BF16),
                pltpu.VMEM((rl * bl, LANES), F32),
                pltpu.VMEM((shells, bl // 2, rl, LANES), F32),
                pltpu.VMEM((LANES, LANES), F32),
                pltpu.VMEM((N, 1, LANES), F32),
                pltpu.VMEM((1, 1, LANES), F32),
                dma, dma((phases, 2 * C)), dma((2 * C - 2,)),
                dma((phases,)), dma((steps,)),
                dma, dma, dma, dma, dma((count,)), dma, dma, dma,
            ],
            compiler_params=pltpu.CompilerParams(
                collective_id=0, has_side_effects=True, vmem_limit_bytes=VMEM_LIMIT
            ),
        )(orient_bin, tilt_slope, particles, interp_table)
        return pl.pallas_call(
            functools.partial(finish, shells),
            out_shape=(
                jax.ShapeDtypeStruct((1, 2, rl, cl), F32),
                jax.ShapeDtypeStruct((2, shells), F32),
                jax.ShapeDtypeStruct((1, shells), F32),
            ),
            in_specs=[vmem, vmem, vmem],
            out_specs=(hbm, hbm, hbm),
            scratch_shapes=[
                pltpu.VMEM((2, shells), F32), pltpu.VMEM((1, shells), F32), dma((3,)),
            ],
            compiler_params=pltpu.CompilerParams(vmem_limit_bytes=FINISH_LIMIT),
        )(maps, spectra, counts)

    placed = (
        P(("half", "row", "col"), None, None, None),
        P(("half", "row", "col")),
        P(("half", "row", "col"), None),
        P(),
    )
    return jax.shard_map(
        local,
        mesh=mesh,
        in_specs=placed,
        out_specs=(P("half", None, "row", "col"), P(), P("half", None)),
        check_vma=False,
    )
```

```python
import functools

import jax
import jax.numpy as jnp
import numpy as np
from jax import lax
from jax.experimental import pallas as pl
from jax.experimental.pallas import tpu as pltpu
from jax.sharding import PartitionSpec as P

F32 = jnp.float32
BF16 = jnp.bfloat16
LANES = 128
VMEM_LIMIT = 60 * 1024 * 1024
FINISH_LIMIT = 4 * 1024 * 1024
MESH = pl.DeviceIdType.MESH


def dot_nt(left, right):
    return lax.dot_general(left, right, (((1,), (1,)), ((), ())), preferred_element_type=F32)


def dot_nn(left, right):
    return lax.dot_general(left, right, (((1,), (0,)), ((), ())), preferred_element_type=F32)


def block_diagonal(block, copies):
    zero = jnp.zeros_like(block)
    rows = [
        jnp.concatenate([block if i == j else zero for j in range(copies)], axis=1)
        for i in range(copies)
    ]
    return jnp.concatenate(rows, axis=0)


def wedge_mask(limit_same, limit_other, grid, lanes):
    centre = grid // 2
    first = lax.broadcasted_iota(jnp.int32, (grid, lanes), 0) - centre
    third = lax.broadcasted_iota(jnp.int32, (grid, lanes), 1) % grid - centre
    limit = jnp.where(first * third >= 0, limit_same, limit_other)
    inside = 16 * jnp.abs(third) <= limit * jnp.abs(first)
    return jnp.where(inside, 1.0, 0.0).astype(BF16)


def shell_counts(grid):
    centre = grid // 2
    wave = np.arange(grid) - centre
    square = wave * wave
    radius = square[:, None, None] + square[None, :, None] + square[None, None, :]
    shell = np.sum([radius >= k * k for k in range(4, centre)], axis=0)
    return np.bincount(shell[radius < centre * centre], minlength=centre - 3)


def part_rows(rl):
    first = max(1, rl // 4)
    return first, (rl - first) // 2, rl - first - (rl - first) // 2


def plan(R, C, turns, portions):
    phases, steps = R.bit_length() - 1, C.bit_length() - 1
    at = {}
    for n, k in enumerate(turns):
        for g in range(2):
            for phase in range(phases):
                at["row", phase, k, g] = 3.0 + 2.2 * n + 3.5 * phase
    for k in turns:
        if k:
            for g in range(2):
                top = k.bit_length()
                ready = [at["row", phases - 1, k, g]]
                ready += [at["col", k | 1 << m, g] for m in range(top, steps)]
                at["col", k, g] = max(ready) + 3.0
    for k in turns[:-1]:
        top = k.bit_length()
        ready = [at["zcol", k | 1 << m] + 5.2 for m in range(top, steps)]
        at["zcol", k] = max(ready + [4.2 if k == turns[0] else 5.2])
    for phase in range(phases):
        at["zrow", phase] = max(at["zcol", 1 << m] for m in range(steps)) + 2.2 * (phase + 1)
    for core, ahead in enumerate((2, 2)):
        for n, k in enumerate(turns[ahead:]):
            at["send", core, k] = at["row", 0, turns[n], 1] + 0.1 + 0.0 * core
    at["numbers",] = 3.2
    for n in range(portions):
        at["work", n] = 5.0 + 1.1 * n
    return sorted(at, key=at.get)


def kernel(
    dims,
    bins_hbm, tilt_hbm, part_hbm, table_hbm,
    maps_ref, spectra_ref,
    part_ref, table_ref, bins_ref, tilt_ref, stage_a, stage_b,
    sums_0, sums_1, sums_z, rows_0, rows_1, rows_z, cols_0, cols_1, cols_z, other_map,
    third_ref, numbers, numbers_in, numbers_s, slab_first, slab_second, wide_second,
    bin_first, bin_second, bin_third, weight,
    inside, stats, stats_in, total,
    sent, recv_row, recv_col, recv_zrow, recv_zcol, recv_num, copy_num,
    recv_stat, recv_half, load_part, load_table, load_bins, load_tilt,
):
    grid, particles, R, C, pitch, bins = dims
    N = R * C
    rl, bl = grid // R, grid // C
    phases, steps = R.bit_length() - 1, C.bit_length() - 1
    half, row, col = lax.axis_index("half"), lax.axis_index("row"), lax.axis_index("col")
    me = row * C + col
    counts = part_rows(rl)
    sums, rows_in, cols_in = (sums_0, sums_1), (rows_0, rows_1), (cols_0, cols_1)

    def peer_id(step):
        peer = (me + step) % N
        return {"row": peer // C, "col": peer % C}

    def flip(index, power):
        return index + (1 - 2 * ((index // power) % 2)) * power

    def power_of(phase, order):
        low, high = 2 ** (phase % phases), 2 ** ((phase + 1) % phases)
        return low + order * (high - low)

    def row_partner(phase, order):
        return {"row": flip(row, power_of(phase, order))}

    def slab_of(index, order):
        slab = row
        for phase in range(phases):
            if (index >> (phases - 1 - phase)) & 1:
                slab = flip(slab, power_of(phase, order))
        return slab

    def col_of(index):
        column = col
        for step in range(steps):
            if (index >> (steps - 1 - step)) & 1:
                column = flip(column, 2 ** step)
        return column

    bins_load = pltpu.make_async_copy(bins_hbm, bins_ref, load_bins)
    tilt_load = pltpu.make_async_copy(tilt_hbm, tilt_ref, load_tilt)
    bins_load.start()
    tilt_load.start()
    table_load = pltpu.make_async_copy(table_hbm, table_ref, load_table)
    table_load.start()
    part_loads = [
        pltpu.make_async_copy(part_hbm.at[p], part_ref.at[p], load_part.at[p])
        for p in range(particles)
    ]
    for copy in part_loads:
        copy.start()

    barrier = pltpu.get_barrier_semaphore()
    for step in range(1, N):
        pl.semaphore_signal(barrier, inc=1, device_id=peer_id(step), device_id_type=MESH)
    pl.semaphore_signal(barrier, inc=1, device_id={"half": 1 - half}, device_id_type=MESH)

    bins_load.wait()
    tilt_load.wait()
    lane = lax.broadcasted_iota(jnp.int32, (1, LANES), 1)
    packed = jnp.zeros((1, LANES), jnp.int32)
    for p in range(particles):
        for i, value in enumerate((bins_ref[p], tilt_ref[p, 0], tilt_ref[p, 1])):
            packed = jnp.where(lane == 3 * p + i, value, packed)
    numbers[0] = packed
    numbers_in[me] = packed

    table_load.wait()
    firsts_, seconds_ = [], []
    for p in range(particles):
        bin_row = bins_ref[p]
        second = table_ref[bin_row, 1].astype(F32)
        for q in range(C):
            slab_second[p, q] = second[q * bl:(q + 1) * bl]
        firsts_.append(table_ref[bin_row, 0])
        seconds_.append(
            jnp.concatenate([slab_second[p, col_of(k)] for k in range(C)], axis=0).astype(BF16)
        )
        third_ref[p * LANES:(p + 1) * LANES, :] = block_diagonal(table_ref[bin_row, 2].T, 2)

    low_lanes = lax.broadcasted_iota(jnp.int32, (grid, LANES), 1) < grid
    for p in range(particles):
        first = firsts_[p]
        mask = wedge_mask(tilt_ref[p, 0], tilt_ref[p, 1], grid, LANES)

        part_loads[p].wait()
        for at in range(grid // 2):
            span = slice(at * LANES, (at + 1) * LANES)
            real, imag = part_ref[p, 0, :, span], part_ref[p, 1, :, span]
            even = jnp.where(low_lanes, real, pltpu.roll(imag, grid, 1)) * mask
            odd = jnp.where(low_lanes, pltpu.roll(real, grid, 1), imag) * mask
            result = dot_nn(first, jnp.concatenate([even, odd], axis=1))
            for o in range(2):
                to = (2 * at + o) * pitch
                stage_a[p, to:to + grid, :] = result[:, o * LANES:(o + 1) * LANES]

    def all_to(src, dst, recv):
        return [
            pltpu.make_async_remote_copy(
                src_ref=src.at[0], dst_ref=dst.at[me], send_sem=sent, recv_sem=recv,
                device_id=peer_id(step), device_id_type=MESH,
            )
            for step in range(1, N)
        ]

    def whole(dst, recv):
        return pltpu.make_async_remote_copy(
            src_ref=dst.at[pl.ds(0, N - 1)], dst_ref=dst.at[pl.ds(0, N - 1)],
            send_sem=sent, recv_sem=recv, device_id=peer_id(1), device_id_type=MESH,
        )

    sent_rows = []

    def remote(src, dst, recv, peer, rows):
        copy = pltpu.make_async_remote_copy(
            src_ref=src, dst_ref=dst, send_sem=sent, recv_sem=recv,
            device_id=peer, device_id_type=MESH,
        )
        return copy, rows

    def zcol_copy(k):
        step = steps - k.bit_length()
        return remote(
            sums_z.at[k], cols_z.at[k], recv_zcol.at[k - 1],
            {"col": flip(col, 2 ** step)}, R * counts[0] * bl,
        )

    def zrow_copy(phase):
        keep = R >> (phase + 1)
        span = pl.ds(keep, keep)
        return remote(
            sums_z.at[0, span], rows_z.at[span], recv_zrow.at[phase],
            row_partner(phase, half), keep * counts[0] * bl,
        )

    def row_copy(phase, k, g):
        keep = R >> (phase + 1)
        span = pl.ds(keep, keep)
        return remote(
            sums[g].at[k, span], rows_in[g].at[k, span], recv_row.at[phase, 2 * k + g],
            row_partner(phase, g), keep * counts[1 + g] * bl,
        )

    def col_copy(k, g):
        step = steps - k.bit_length()
        return remote(
            sums[g].at[k, 0], cols_in[g].at[k], recv_col.at[2 * k + g - 2],
            {"col": flip(col, 2 ** step)}, counts[1 + g] * bl,
        )

    def start(message):
        message[0].start()
        sent_rows.append(message[1])

    def start_on(core, k):
        messages = [row_copy(0, k, g) for g in range(2)]
        if core == 0:
            sent_rows.extend(rows for _, rows in messages)

        @pl.when(half == core)
        def _():
            for copy, _ in messages:
                copy.start()

    firsts_of = [0, R * counts[0], R * (counts[0] + counts[1])]
    within = [0, counts[0], counts[0] + counts[1]]

    def along_second(parts):
        places = [
            (firsts_of[g] + j * counts[g] + i, slab_of(j, order) * rl + within[g] + i)
            for g, order, j0, j1 in parts
            for j in range(j0, j1)
            for i in range(counts[g])
        ]
        for n in range(0, len(places), 2):
            pair = places[n:n + 2]
            for p in range(particles):
                block = jnp.concatenate(
                    [stage_a[p, pl.ds(a, grid, stride=pitch), :] for _, a in pair], axis=1
                ).astype(BF16)
                result = dot_nn(seconds_[p], block).astype(stage_b.dtype)
                for i, (to, _) in enumerate(pair):
                    for k in range(C):
                        stage_b[p, k, to] = result[
                            k * bl:(k + 1) * bl, i * LANES:(i + 1) * LANES
                        ]

    def along_third(parts):
        pieces, places = [], []
        for to, k, g, j0, j1 in parts:
            rows = counts[g] * bl
            low, high = (firsts_of[g] + j * counts[g] for j in (j0, j1))
            pieces.append(jnp.concatenate(
                [
                    stage_b[p, k, low:high].reshape((high - low) * bl, LANES)
                    for p in range(particles)
                ],
                axis=1,
            ))
            places += [(to, k, j, rows) for j in range(j0, j1)]
        result = dot_nn(jnp.concatenate(pieces, axis=0).astype(BF16), third_ref[...])
        at = 0
        for to, k, j, rows in places:
            to[k, j] = result[at:at + rows]
            at += rows

    def row_parts(turn, j0, j1):
        return [(sums[g], k, 1 + g, j0, j1) for k in turn for g in range(2)]

    turns = sorted(
        range(C), key=lambda k: -sum(((k >> i) & 1) << (steps - 1 - i) for i in range(steps))
    )
    along_second([(1 + g, g, R // 2, R) for g in range(2)] + [(0, half, 0, R)])
    along_third(row_parts(turns[:1], R // 2, R) + [(sums_z, k, 0, 0, R) for k in range(C // 2, C)])
    pl.semaphore_wait(barrier, N)
    for copy in all_to(numbers, numbers_in, recv_num):
        copy.start()
    for g in range(2):
        start(row_copy(0, turns[0], g))
    for k in [k for k in turns if k >= C // 2]:
        start(zcol_copy(k))
    along_third(row_parts(turns[1:], R // 2, R))
    start_on(0, turns[1])
    start_on(1, turns[1])
    along_second([(1 + g, g, 0, R // 2) for g in range(2)])
    along_third(row_parts(turns, 0, R // 2) + [(sums_z, k, 0, 0, R) for k in range(C // 2)])

    local = pltpu.make_async_copy(numbers_in, numbers_s, copy_num)
    weight[...] = jnp.zeros_like(weight)
    ones = jnp.ones((grid, LANES), BF16)

    def bin_tables(n, carry):
        first = table_ref[n, 0].astype(F32)
        second = dot_nn(table_ref[n, 1], ones)
        for r in range(R):
            slab_first[0, r] = first[r * rl:(r + 1) * rl]
        for q in range(C):
            wide_second[q] = second[q * bl:(q + 1) * bl]
        bin_first[n] = slab_first[0, row]
        bin_second[n] = wide_second[col]
        across = table_ref[n, 2].T
        bin_third[n] = jnp.concatenate([across, across], axis=1)
        return carry

    lax.fori_loop(0, bins, bin_tables, 0, unroll=4)

    together = 2
    first_wave = lax.broadcasted_iota(jnp.int32, (grid, LANES), 0) - grid // 2
    third_wave = lax.broadcasted_iota(jnp.int32, (grid, LANES), 1) % grid - grid // 2
    same_side = first_wave * third_wave >= 0
    first_size, third_size = jnp.abs(first_wave), 16 * jnp.abs(third_wave)
    low_rows = lax.broadcasted_iota(jnp.int32, (rl, LANES), 1) < grid
    low_seconds = lax.broadcasted_iota(jnp.int32, (bl, LANES), 1) < grid

    def add_weight(step, carry):
        members = [(step * together + n, p) for n in range(together) for p in range(particles)]
        blocks, thirds = [], []
        for i in range(0, len(members), 2):
            numbers_of = [
                [numbers_s[n, 0, 3 * p + v] for v in range(3)] for n, p in members[i:i + 2]
            ]
            limit = jnp.where(
                same_side,
                jnp.where(low_lanes, numbers_of[0][1], numbers_of[1][1]),
                jnp.where(low_lanes, numbers_of[0][2], numbers_of[1][2]),
            )
            mask = jnp.where(third_size <= limit * first_size, 1.0, 0.0).astype(BF16)
            along = [dot_nn(bin_first[value[0]].astype(BF16), mask) for value in numbers_of]
            first = jnp.where(low_rows, along[0], along[1]).astype(BF16).astype(F32)
            second = jnp.where(
                low_seconds, bin_second[numbers_of[0][0]], bin_second[numbers_of[1][0]]
            )
            blocks.append(
                jnp.concatenate([first[a:a + 1] * second for a in range(rl)], axis=0).astype(BF16)
            )
            thirds += [bin_third[value[0]] for value in numbers_of]
        weight[...] += dot_nn(jnp.concatenate(blocks, axis=1), jnp.concatenate(thirds, axis=0))
        return carry

    centre = grid // 2
    shells = centre - 3
    tile_rows = lax.broadcasted_iota(jnp.int32, (rl, LANES), 0)
    tile_lanes = lax.broadcasted_iota(jnp.int32, (rl, LANES), 1)
    wave_first = row * rl + tile_rows - centre
    wave_third = tile_lanes % grid - centre
    fixed = wave_first * wave_first + wave_third * wave_third
    radius = []
    for pair in range(bl // 2):
        wave_second = col * bl + 2 * pair + tile_lanes // grid - centre
        radius.append(fixed + wave_second * wave_second)
    for s in range(shells):
        least = (s + 3) * (s + 3) if s else 0
        beyond = (s + 4) * (s + 4)
        for pair, r2 in enumerate(radius):
            inside[s, pair] = jnp.where((r2 >= least) & (r2 < beyond), 1.0, 0.0)

    groups = N // together
    portions = 8
    done = set()
    worked = [0]

    def work():
        n = worked[0]
        worked[0] = n + 1
        if n == 0:
            local.wait()
        low, high = groups * n // portions, groups * (n + 1) // portions
        if high > low:
            lax.fori_loop(low, high, add_weight, 0)

    def col_ready(k, g):
        top = k.bit_length()
        return all(("row", phases - 1, k, g) in done and ("col", k | 1 << m, g) in done for m in range(top, steps)) and ("row", phases - 1, k, g) in done

    def maybe_col(k, g):
        if k and col_ready(k, g) and ("sentcol", k, g) not in done:
            done.add(("sentcol", k, g))
            start(col_copy(k, g))

    def take(event):
        kind = event[0]
        if kind == "work":
            work()
            return
        if kind == "send":
            start_on(*event[1:])
            return
        if kind == "numbers":
            whole(numbers_in, recv_num).wait_recv()
            local.start()
            return
        if kind == "zcol":
            zcol_copy(event[1])[0].wait_recv()
        elif kind == "zrow":
            zrow_copy(event[1])[0].wait_recv()
        elif kind == "row":
            row_copy(*event[1:])[0].wait_recv()
        else:
            col_copy(*event[1:])[0].wait_recv()
        done.add(event)
        if kind == "zcol":
            k = event[1]
            into = k - (1 << k.bit_length() - 1)
            sums_z[into] = sums_z[into] + cols_z[k]
            if all(("zcol", into | 1 << m) in done for m in range(into.bit_length(), steps)):
                start(zcol_copy(into) if into else zrow_copy(0))
        elif kind == "zrow":
            phase = event[1]
            keep = R >> (phase + 1)
            sums_z[0, :keep] = sums_z[0, :keep] + rows_z[keep:2 * keep]
            if phase + 1 < phases:
                start(zrow_copy(phase + 1))
        elif kind == "row":
            _, phase, k, g = event
            keep = R >> (phase + 1)
            sums[g][k, :keep] = sums[g][k, :keep] + rows_in[g][k, keep:2 * keep]
            if phase + 1 < phases:
                start(row_copy(phase + 1, k, g))
            else:
                maybe_col(k, g)
        else:
            _, k, g = event
            into = k - (1 << k.bit_length() - 1)
            sums[g][into, 0] = sums[g][into, 0] + cols_in[g][k]
            maybe_col(into, g)

    for event in plan(R, C, turns, portions):
        take(event)

    block = jnp.concatenate([sums_z[0, 0], sums_0[0, 0], sums_1[0, 0]], axis=0)
    weight[...] = block / (weight[...] + 1.0)
    low = lax.broadcasted_iota(jnp.int32, (rl, LANES), 1) < grid
    for pair in range(bl // 2):
        span = slice(pair * LANES, (pair + 1) * LANES)
        even, odd = (weight[pl.ds(2 * pair + i, rl, stride=bl), :] for i in range(2))
        maps_ref[0, 0, :, span] = jnp.where(low, even, pltpu.roll(odd, grid, 1))
        maps_ref[0, 1, :, span] = jnp.where(low, pltpu.roll(even, grid, 1), odd)

    half_copy = pltpu.make_async_remote_copy(
        src_ref=maps_ref.at[0], dst_ref=other_map, send_sem=sent, recv_sem=recv_half,
        device_id={"half": 1 - half}, device_id_type=MESH,
    )
    half_copy.start()
    stats[...] = jnp.zeros_like(stats)

    def shell_sums(rows_at, values):
        for s in range(shells):
            parts = [jnp.zeros((rl, LANES), F32) for _ in values]
            for pair in range(bl // 2):
                mask = inside[s, pair]
                parts = [part + mask * value[pair] for part, value in zip(parts, values)]
            for at, part in zip(rows_at, parts):
                stats[pl.ds(at + s, 1), :] = jnp.sum(part, axis=0, keepdims=True)

    def tiles(ref, c):
        return [ref[c, :, pair * LANES:(pair + 1) * LANES] for pair in range(bl // 2)]

    mine = [tiles(maps_ref.at[0], c) for c in range(2)]
    shell_sums([32 + 32 * half], [[x * x + y * y for x, y in zip(*mine)]])
    half_copy.wait_recv()
    theirs = [tiles(other_map, c) for c in range(2)]
    mine = [tiles(maps_ref.at[0], c) for c in range(2)]
    shell_sums(
        [0, 64 - 32 * half],
        [
            [x * u + y * v for x, y, u, v in zip(*mine, *theirs)],
            [u * u + v * v for u, v in zip(*theirs)],
        ],
    )
    mine = jnp.sum(stats[...].T, axis=0, keepdims=True)
    total[0] = mine
    stats_in[me] = mine
    for copy in all_to(total, stats_in, recv_stat):
        copy.start()
    whole(stats_in, recv_stat).wait_recv()
    spectra = stats_in[0]
    for n in range(1, N):
        spectra = spectra + stats_in[n]
    spectra_ref[...] = spectra
    rows = sum(sent_rows) + 2 * (N - 1) + 2 * rl * bl * grid // LANES
    everything = stage_a.at[0, pl.ds(0, rows)]
    pltpu.make_async_remote_copy(
        src_ref=everything, dst_ref=everything, send_sem=sent, recv_sem=recv_half,
        device_id={"half": 1 - half}, device_id_type=MESH,
    ).wait_send()


def finish(shells, maps_in, spectra_ref, counts_ref, maps, power, corr, power_ref, corr_ref, done):
    maps_out = pltpu.make_async_copy(maps_in, maps, done.at[0])
    maps_out.start()
    spectra = spectra_ref[...]
    cross = spectra[:, 0:shells]
    power_first = spectra[:, 32:32 + shells]
    power_second = spectra[:, 64:64 + shells]
    power_ref[0:1, :] = power_first / counts_ref[...]
    power_ref[1:2, :] = power_second / counts_ref[...]
    corr_ref[...] = cross / jnp.sqrt(power_first * power_second + 1e-6)
    small = [
        pltpu.make_async_copy(power_ref, power, done.at[1]),
        pltpu.make_async_copy(corr_ref, corr, done.at[2]),
    ]
    for copy in small:
        copy.start()
    for copy in [maps_out] + small:
        copy.wait()


def solution(mesh):
    R, C = mesh.shape["row"], mesh.shape["col"]
    N = R * C

    def local(particles, orient_bin, tilt_slope, interp_table):
        count, _, grid, plane = particles.shape
        rl, cl, bl = grid // R, plane // C, grid // C
        shells = grid // 2 - 3
        phases = R.bit_length() - 1
        pitch = grid + 8
        bins = interp_table.shape[0]
        steps = C.bit_length() - 1
        nz, n0, n1 = part_rows(rl)
        counts = jnp.asarray(shell_counts(grid)[None], F32)
        vmem, hbm = pl.BlockSpec(memory_space=pltpu.VMEM), pl.BlockSpec(memory_space=pltpu.HBM)
        dma = pltpu.SemaphoreType.DMA
        maps, spectra = pl.pallas_call(
            functools.partial(kernel, (grid, count, R, C, pitch, bins)),
            out_shape=(
                pltpu.VMEM((1, 2, rl, cl), F32),
                pltpu.VMEM((1, LANES), F32),
            ),
            in_specs=[hbm, hbm, hbm, hbm],
            out_specs=(vmem, vmem),
            scratch_shapes=[
                pltpu.VMEM(particles.shape, particles.dtype),
                pltpu.VMEM(interp_table.shape, interp_table.dtype),
                pltpu.SMEM(orient_bin.shape, jnp.int32),
                pltpu.SMEM(tilt_slope.shape, jnp.int32),
                pltpu.VMEM((count, grid * pitch, LANES), F32),
                pltpu.VMEM((count, C, grid, bl, LANES), F32 if bl % 16 else BF16),
                pltpu.VMEM((C, R, n0 * bl, LANES), F32),
                pltpu.VMEM((C, R, n1 * bl, LANES), F32),
                pltpu.VMEM((C, R, nz * bl, LANES), F32),
                pltpu.VMEM((C, R, n0 * bl, LANES), F32),
                pltpu.VMEM((C, R, n1 * bl, LANES), F32),
                pltpu.VMEM((R, nz * bl, LANES), F32),
                pltpu.VMEM((C, n0 * bl, LANES), F32),
                pltpu.VMEM((C, n1 * bl, LANES), F32),
                pltpu.VMEM((C, R, nz * bl, LANES), F32),
                pltpu.VMEM((2, rl, cl), F32),
                pltpu.VMEM((count * LANES, LANES), BF16),
                pltpu.VMEM((1, 1, LANES), jnp.int32),
                pltpu.VMEM((N, 1, LANES), jnp.int32),
                pltpu.SMEM((N, 1, LANES), jnp.int32),
                pltpu.VMEM((count, R, rl, grid), F32),
                pltpu.VMEM((count, C, bl, grid), F32),
                pltpu.VMEM((C, bl, LANES), F32),
                pltpu.VMEM((bins, rl, grid), F32),
                pltpu.VMEM((bins, bl, LANES), F32),
                pltpu.VMEM((bins, grid, LANES), BF16),
                pltpu.VMEM((rl * bl, LANES), F32),
                pltpu.VMEM((shells, bl // 2, rl, LANES), F32),
                pltpu.VMEM((LANES, LANES), F32),
                pltpu.VMEM((N, 1, LANES), F32),
                pltpu.VMEM((1, 1, LANES), F32),
                dma, dma((phases, 2 * C)), dma((2 * C - 2,)),
                dma((phases,)), dma((C - 1,)),
                dma, dma, dma, dma, dma((count,)), dma, dma, dma,
            ],
            compiler_params=pltpu.CompilerParams(
                collective_id=0, has_side_effects=True, vmem_limit_bytes=VMEM_LIMIT
            ),
        )(orient_bin, tilt_slope, particles, interp_table)
        return pl.pallas_call(
            functools.partial(finish, shells),
            out_shape=(
                jax.ShapeDtypeStruct((1, 2, rl, cl), F32),
                jax.ShapeDtypeStruct((2, shells), F32),
                jax.ShapeDtypeStruct((1, shells), F32),
            ),
            in_specs=[vmem, vmem, vmem],
            out_specs=(hbm, hbm, hbm),
            scratch_shapes=[
                pltpu.VMEM((2, shells), F32), pltpu.VMEM((1, shells), F32), dma((3,)),
            ],
            compiler_params=pltpu.CompilerParams(vmem_limit_bytes=FINISH_LIMIT),
        )(maps, spectra, counts)

    placed = (
        P(("half", "row", "col"), None, None, None),
        P(("half", "row", "col")),
        P(("half", "row", "col"), None),
        P(),
    )
    return jax.shard_map(
        local,
        mesh=mesh,
        in_specs=placed,
        out_specs=(P("half", None, "row", "col"), P(), P("half", None)),
        check_vma=False,
    )
```

```python
import functools

import jax
import jax.numpy as jnp
import numpy as np
from jax import lax
from jax.experimental import pallas as pl
from jax.experimental.pallas import tpu as pltpu
from jax.sharding import PartitionSpec as P

F32 = jnp.float32
BF16 = jnp.bfloat16
LANES = 128
VMEM_LIMIT = 60 * 1024 * 1024
FINISH_LIMIT = 4 * 1024 * 1024
MESH = pl.DeviceIdType.MESH


def dot_nt(left, right):
    return lax.dot_general(left, right, (((1,), (1,)), ((), ())), preferred_element_type=F32)


def dot_nn(left, right):
    return lax.dot_general(left, right, (((1,), (0,)), ((), ())), preferred_element_type=F32)


def block_diagonal(block, copies):
    zero = jnp.zeros_like(block)
    rows = [
        jnp.concatenate([block if i == j else zero for j in range(copies)], axis=1)
        for i in range(copies)
    ]
    return jnp.concatenate(rows, axis=0)


def wedge_mask(limit_same, limit_other, grid, lanes):
    centre = grid // 2
    first = lax.broadcasted_iota(jnp.int32, (grid, lanes), 0) - centre
    third = lax.broadcasted_iota(jnp.int32, (grid, lanes), 1) % grid - centre
    limit = jnp.where(first * third >= 0, limit_same, limit_other)
    inside = 16 * jnp.abs(third) <= limit * jnp.abs(first)
    return jnp.where(inside, 1.0, 0.0).astype(BF16)


def shell_counts(grid):
    centre = grid // 2
    wave = np.arange(grid) - centre
    square = wave * wave
    radius = square[:, None, None] + square[None, :, None] + square[None, None, :]
    shell = np.sum([radius >= k * k for k in range(4, centre)], axis=0)
    return np.bincount(shell[radius < centre * centre], minlength=centre - 3)


def part_rows(rl):
    first = max(1, rl // 4)
    return first, (rl - first) // 2, rl - first - (rl - first) // 2


def plan(R, C, turns, portions):
    phases, steps = R.bit_length() - 1, C.bit_length() - 1
    at = {}
    for n, k in enumerate(turns):
        for g in range(2):
            for phase in range(phases):
                at["row", phase, k, g] = 3.0 + 2.2 * n + 3.5 * phase
    for k in turns:
        if k:
            for g in range(2):
                top = k.bit_length()
                ready = [at["row", phases - 1, k, g]]
                ready += [at["col", k | 1 << m, g] for m in range(top, steps)]
                at["col", k, g] = max(ready) + 3.0
    for k in turns[:-1]:
        top = k.bit_length()
        ready = [at["zcol", k | 1 << m] + 5.2 for m in range(top, steps)]
        at["zcol", k] = max(ready + [4.2 if k == turns[0] else 5.2])
    for phase in range(phases):
        at["zrow", phase] = max(at["zcol", 1 << m] for m in range(steps)) + 2.2 * (phase + 1)
    for core, ahead in enumerate((2, 2)):
        for n, k in enumerate(turns[ahead:]):
            at["send", core, k] = at["row", 0, turns[n], 1] + 0.1 + 0.0 * core
    at["numbers",] = 3.2
    for n in range(portions):
        at["work", n] = 5.0 + 1.1 * n
    return sorted(at, key=at.get)


def kernel(
    dims,
    bins_hbm, tilt_hbm, part_hbm, table_hbm,
    maps_ref, spectra_ref,
    part_ref, first_ref, table_ref, bins_ref, tilt_ref, stage_a, stage_b,
    sums_0, sums_1, sums_z, rows_0, rows_1, rows_z, cols_0, cols_1, cols_z, other_map,
    third_ref, numbers, numbers_in, numbers_s, slab_first, slab_second, wide_second,
    bin_first, bin_second, bin_third, weight,
    inside, stats, stats_in, total,
    sent, recv_row, recv_col, recv_zrow, recv_zcol, recv_num, copy_num,
    recv_stat, recv_half, recv_power, load_part, load_first, load_table, load_bins, load_tilt,
):
    grid, particles, R, C, pitch, bins = dims
    N = R * C
    rl, bl = grid // R, grid // C
    phases, steps = R.bit_length() - 1, C.bit_length() - 1
    half, row, col = lax.axis_index("half"), lax.axis_index("row"), lax.axis_index("col")
    me = row * C + col
    counts = part_rows(rl)
    sums, rows_in, cols_in = (sums_0, sums_1), (rows_0, rows_1), (cols_0, cols_1)

    def peer_id(step):
        peer = (me + step) % N
        return {"row": peer // C, "col": peer % C}

    def flip(index, power):
        return index + (1 - 2 * ((index // power) % 2)) * power

    def power_of(phase, order):
        low, high = 2 ** (phase % phases), 2 ** ((phase + 1) % phases)
        return low + order * (high - low)

    def row_partner(phase, order):
        return {"row": flip(row, power_of(phase, order))}

    def slab_of(index, order):
        slab = row
        for phase in range(phases):
            if (index >> (phases - 1 - phase)) & 1:
                slab = flip(slab, power_of(phase, order))
        return slab

    def col_of(index):
        column = col
        for step in range(steps):
            if (index >> (steps - 1 - step)) & 1:
                column = flip(column, 2 ** step)
        return column

    bins_load = pltpu.make_async_copy(bins_hbm, bins_ref, load_bins)
    tilt_load = pltpu.make_async_copy(tilt_hbm, tilt_ref, load_tilt)
    bins_load.start()
    tilt_load.start()
    first_load = pltpu.make_async_copy(table_hbm.at[:, 0], first_ref, load_first)
    first_load.start()
    part_loads = [
        pltpu.make_async_copy(part_hbm.at[p], part_ref.at[p], load_part.at[p])
        for p in range(particles)
    ]
    for copy in part_loads:
        copy.start()
    table_load = pltpu.make_async_copy(
        table_hbm.at[:, pl.ds(1, 2)], table_ref, load_table
    )
    table_load.start()

    barrier = pltpu.get_barrier_semaphore()
    for step in range(1, N):
        pl.semaphore_signal(barrier, inc=1, device_id=peer_id(step), device_id_type=MESH)
    pl.semaphore_signal(barrier, inc=1, device_id={"half": 1 - half}, device_id_type=MESH)

    bins_load.wait()
    tilt_load.wait()
    lane = lax.broadcasted_iota(jnp.int32, (1, LANES), 1)
    packed = jnp.zeros((1, LANES), jnp.int32)
    for p in range(particles):
        for i, value in enumerate((bins_ref[p], tilt_ref[p, 0], tilt_ref[p, 1])):
            packed = jnp.where(lane == 3 * p + i, value, packed)
    numbers[0] = packed
    numbers_in[me] = packed

    first_load.wait()
    firsts_ = [first_ref[bins_ref[p]] for p in range(particles)]

    def later_tables():
        table_load.wait()
        seconds = []
        for p in range(particles):
            bin_row = bins_ref[p]
            second = table_ref[bin_row, 0].astype(F32)
            for q in range(C):
                slab_second[p, q] = second[q * bl:(q + 1) * bl]
            seconds.append(
                jnp.concatenate([slab_second[p, col_of(k)] for k in range(C)], axis=0).astype(BF16)
            )
            third_ref[p * LANES:(p + 1) * LANES, :] = block_diagonal(table_ref[bin_row, 1].T, 2)
        return seconds

    for copy in part_loads:
        copy.wait()
    low_lanes = lax.broadcasted_iota(jnp.int32, (grid, LANES), 1) < grid
    for p in range(particles):
        first = firsts_[p]
        mask = wedge_mask(tilt_ref[p, 0], tilt_ref[p, 1], grid, LANES)

        for at in range(grid // 2):
            span = slice(at * LANES, (at + 1) * LANES)
            real, imag = part_ref[p, 0, :, span], part_ref[p, 1, :, span]
            even = jnp.where(low_lanes, real, pltpu.roll(imag, grid, 1)) * mask
            odd = jnp.where(low_lanes, pltpu.roll(real, grid, 1), imag) * mask
            result = dot_nn(first, jnp.concatenate([even, odd], axis=1))
            for o in range(2):
                to = (2 * at + o) * pitch
                stage_a[p, to:to + grid, :] = result[:, o * LANES:(o + 1) * LANES]

    seconds_ = later_tables()

    def all_to(src, dst, recv):
        return [
            pltpu.make_async_remote_copy(
                src_ref=src.at[0], dst_ref=dst.at[me], send_sem=sent, recv_sem=recv,
                device_id=peer_id(step), device_id_type=MESH,
            )
            for step in range(1, N)
        ]

    def whole(dst, recv):
        return pltpu.make_async_remote_copy(
            src_ref=dst.at[pl.ds(0, N - 1)], dst_ref=dst.at[pl.ds(0, N - 1)],
            send_sem=sent, recv_sem=recv, device_id=peer_id(1), device_id_type=MESH,
        )

    sent_rows = []

    def remote(src, dst, recv, peer, rows):
        copy = pltpu.make_async_remote_copy(
            src_ref=src, dst_ref=dst, send_sem=sent, recv_sem=recv,
            device_id=peer, device_id_type=MESH,
        )
        return copy, rows

    def zcol_copy(k):
        step = steps - k.bit_length()
        return remote(
            sums_z.at[k], cols_z.at[k], recv_zcol.at[k - 1],
            {"col": flip(col, 2 ** step)}, R * counts[0] * bl,
        )

    def zrow_copy(phase):
        keep = R >> (phase + 1)
        span = pl.ds(keep, keep)
        return remote(
            sums_z.at[0, span], rows_z.at[span], recv_zrow.at[phase],
            row_partner(phase, half), keep * counts[0] * bl,
        )

    def row_copy(phase, k, g):
        keep = R >> (phase + 1)
        span = pl.ds(keep, keep)
        return remote(
            sums[g].at[k, span], rows_in[g].at[k, span], recv_row.at[phase, 2 * k + g],
            row_partner(phase, g), keep * counts[1 + g] * bl,
        )

    def col_copy(k, g):
        step = steps - k.bit_length()
        return remote(
            sums[g].at[k, 0], cols_in[g].at[k], recv_col.at[2 * k + g - 2],
            {"col": flip(col, 2 ** step)}, counts[1 + g] * bl,
        )

    def start(message):
        message[0].start()
        sent_rows.append(message[1])

    def start_on(core, k):
        messages = [row_copy(0, k, g) for g in range(2)]
        if core == 0:
            sent_rows.extend(rows for _, rows in messages)

        @pl.when(half == core)
        def _():
            for copy, _ in messages:
                copy.start()

    firsts_of = [0, R * counts[0], R * (counts[0] + counts[1])]
    within = [0, counts[0], counts[0] + counts[1]]

    def along_second(parts):
        places = [
            (firsts_of[g] + j * counts[g] + i, slab_of(j, order) * rl + within[g] + i)
            for g, order, j0, j1 in parts
            for j in range(j0, j1)
            for i in range(counts[g])
        ]
        for n in range(0, len(places), 2):
            pair = places[n:n + 2]
            for p in range(particles):
                block = jnp.concatenate(
                    [stage_a[p, pl.ds(a, grid, stride=pitch), :] for _, a in pair], axis=1
                ).astype(BF16)
                result = dot_nn(seconds_[p], block).astype(stage_b.dtype)
                for i, (to, _) in enumerate(pair):
                    for k in range(C):
                        stage_b[p, k, to] = result[
                            k * bl:(k + 1) * bl, i * LANES:(i + 1) * LANES
                        ]

    def along_third(parts):
        pieces, places = [], []
        for to, k, g, j0, j1 in parts:
            rows = counts[g] * bl
            low, high = (firsts_of[g] + j * counts[g] for j in (j0, j1))
            pieces.append(jnp.concatenate(
                [
                    stage_b[p, k, low:high].reshape((high - low) * bl, LANES)
                    for p in range(particles)
                ],
                axis=1,
            ))
            places += [(to, k, j, rows) for j in range(j0, j1)]
        result = dot_nn(jnp.concatenate(pieces, axis=0).astype(BF16), third_ref[...])
        at = 0
        for to, k, j, rows in places:
            to[k, j] = result[at:at + rows]
            at += rows

    def row_parts(turn, j0, j1):
        return [(sums[g], k, 1 + g, j0, j1) for k in turn for g in range(2)]

    turns = sorted(
        range(C), key=lambda k: -sum(((k >> i) & 1) << (steps - 1 - i) for i in range(steps))
    )
    along_second([(1 + g, g, R // 2, R) for g in range(2)] + [(0, half, 0, R)])
    along_third(row_parts(turns[:1], R // 2, R) + [(sums_z, k, 0, 0, R) for k in range(C // 2, C)])
    pl.semaphore_wait(barrier, N)
    for copy in all_to(numbers, numbers_in, recv_num):
        copy.start()
    for g in range(2):
        start(row_copy(0, turns[0], g))
    for k in [k for k in turns if k >= C // 2]:
        start(zcol_copy(k))
    along_third(row_parts(turns[1:], R // 2, R))
    start_on(0, turns[1])
    start_on(1, turns[1])
    along_second([(1 + g, g, 0, R // 2) for g in range(2)])
    along_third(row_parts(turns, 0, R // 2) + [(sums_z, k, 0, 0, R) for k in range(C // 2)])

    local = pltpu.make_async_copy(numbers_in, numbers_s, copy_num)
    weight[...] = jnp.zeros_like(weight)
    ones = jnp.ones((grid, LANES), BF16)

    def bin_tables(n, carry):
        first = first_ref[n].astype(F32)
        second = dot_nn(table_ref[n, 0], ones)
        for r in range(R):
            slab_first[0, r] = first[r * rl:(r + 1) * rl]
        for q in range(C):
            wide_second[q] = second[q * bl:(q + 1) * bl]
        bin_first[n] = slab_first[0, row]
        bin_second[n] = wide_second[col]
        across = table_ref[n, 1].T
        bin_third[n] = jnp.concatenate([across, across], axis=1)
        return carry

    lax.fori_loop(0, bins, bin_tables, 0, unroll=4)

    together = 2
    first_wave = lax.broadcasted_iota(jnp.int32, (grid, LANES), 0) - grid // 2
    third_wave = lax.broadcasted_iota(jnp.int32, (grid, LANES), 1) % grid - grid // 2
    same_side = first_wave * third_wave >= 0
    first_size, third_size = jnp.abs(first_wave), 16 * jnp.abs(third_wave)
    low_rows = lax.broadcasted_iota(jnp.int32, (rl, LANES), 1) < grid
    low_seconds = lax.broadcasted_iota(jnp.int32, (bl, LANES), 1) < grid

    def add_weight(step, carry):
        members = [(step * together + n, p) for n in range(together) for p in range(particles)]
        blocks, thirds = [], []
        for i in range(0, len(members), 2):
            numbers_of = [
                [numbers_s[n, 0, 3 * p + v] for v in range(3)] for n, p in members[i:i + 2]
            ]
            limit = jnp.where(
                same_side,
                jnp.where(low_lanes, numbers_of[0][1], numbers_of[1][1]),
                jnp.where(low_lanes, numbers_of[0][2], numbers_of[1][2]),
            )
            mask = jnp.where(third_size <= limit * first_size, 1.0, 0.0).astype(BF16)
            along = [dot_nn(bin_first[value[0]].astype(BF16), mask) for value in numbers_of]
            first = jnp.where(low_rows, along[0], along[1]).astype(BF16).astype(F32)
            second = jnp.where(
                low_seconds, bin_second[numbers_of[0][0]], bin_second[numbers_of[1][0]]
            )
            blocks.append(
                jnp.concatenate([first[a:a + 1] * second for a in range(rl)], axis=0).astype(BF16)
            )
            thirds += [bin_third[value[0]] for value in numbers_of]
        weight[...] += dot_nn(jnp.concatenate(blocks, axis=1), jnp.concatenate(thirds, axis=0))
        return carry

    centre = grid // 2
    shells = centre - 3
    tile_rows = lax.broadcasted_iota(jnp.int32, (rl, LANES), 0)
    tile_lanes = lax.broadcasted_iota(jnp.int32, (rl, LANES), 1)
    wave_first = row * rl + tile_rows - centre
    wave_third = tile_lanes % grid - centre
    fixed = wave_first * wave_first + wave_third * wave_third
    radius = []
    for pair in range(bl // 2):
        wave_second = col * bl + 2 * pair + tile_lanes // grid - centre
        radius.append(fixed + wave_second * wave_second)
    for s in range(shells):
        least = (s + 3) * (s + 3) if s else 0
        beyond = (s + 4) * (s + 4)
        for pair, r2 in enumerate(radius):
            inside[s, pair] = jnp.where((r2 >= least) & (r2 < beyond), 1.0, 0.0)

    groups = N // together
    portions = 8
    done = set()
    worked = [0]

    def work():
        n = worked[0]
        worked[0] = n + 1
        if n == 0:
            local.wait()
        low, high = groups * n // portions, groups * (n + 1) // portions
        if high > low:
            lax.fori_loop(low, high, add_weight, 0)

    def col_ready(k, g):
        top = k.bit_length()
        return all(("row", phases - 1, k, g) in done and ("col", k | 1 << m, g) in done for m in range(top, steps)) and ("row", phases - 1, k, g) in done

    def maybe_col(k, g):
        if k and col_ready(k, g) and ("sentcol", k, g) not in done:
            done.add(("sentcol", k, g))
            start(col_copy(k, g))

    def take(event):
        kind = event[0]
        if kind == "work":
            work()
            return
        if kind == "send":
            start_on(*event[1:])
            return
        if kind == "numbers":
            whole(numbers_in, recv_num).wait_recv()
            local.start()
            return
        if kind == "zcol":
            zcol_copy(event[1])[0].wait_recv()
        elif kind == "zrow":
            zrow_copy(event[1])[0].wait_recv()
        elif kind == "row":
            row_copy(*event[1:])[0].wait_recv()
        else:
            col_copy(*event[1:])[0].wait_recv()
        done.add(event)
        if kind == "zcol":
            k = event[1]
            into = k - (1 << k.bit_length() - 1)
            sums_z[into] = sums_z[into] + cols_z[k]
            if all(("zcol", into | 1 << m) in done for m in range(into.bit_length(), steps)):
                start(zcol_copy(into) if into else zrow_copy(0))
        elif kind == "zrow":
            phase = event[1]
            keep = R >> (phase + 1)
            sums_z[0, :keep] = sums_z[0, :keep] + rows_z[keep:2 * keep]
            if phase + 1 < phases:
                start(zrow_copy(phase + 1))
        elif kind == "row":
            _, phase, k, g = event
            keep = R >> (phase + 1)
            sums[g][k, :keep] = sums[g][k, :keep] + rows_in[g][k, keep:2 * keep]
            if phase + 1 < phases:
                start(row_copy(phase + 1, k, g))
            else:
                maybe_col(k, g)
        else:
            _, k, g = event
            into = k - (1 << k.bit_length() - 1)
            sums[g][into, 0] = sums[g][into, 0] + cols_in[g][k]
            maybe_col(into, g)

    for event in plan(R, C, turns, portions):
        take(event)

    block = jnp.concatenate([sums_z[0, 0], sums_0[0, 0], sums_1[0, 0]], axis=0)
    weight[...] = block / (weight[...] + 1.0)
    low = lax.broadcasted_iota(jnp.int32, (rl, LANES), 1) < grid
    for pair in range(bl // 2):
        span = slice(pair * LANES, (pair + 1) * LANES)
        even, odd = (weight[pl.ds(2 * pair + i, rl, stride=bl), :] for i in range(2))
        maps_ref[0, 0, :, span] = jnp.where(low, even, pltpu.roll(odd, grid, 1))
        maps_ref[0, 1, :, span] = jnp.where(low, pltpu.roll(even, grid, 1), odd)

    half_copy = pltpu.make_async_remote_copy(
        src_ref=maps_ref.at[0], dst_ref=other_map, send_sem=sent, recv_sem=recv_half,
        device_id={"half": 1 - half}, device_id_type=MESH,
    )
    half_copy.start()
    own_rows = pl.ds(pl.multiple_of(32 + 32 * half, 32), 32)
    for rows in (pl.ds(0, 32), own_rows, pl.ds(96, 32)):
        stats[rows] = jnp.zeros((32, LANES), F32)

    def shell_sums(rows_at, values):
        for s in range(shells):
            parts = [jnp.zeros((rl, LANES), F32) for _ in values]
            for pair in range(bl // 2):
                mask = inside[s, pair]
                parts = [part + mask * value[pair] for part, value in zip(parts, values)]
            for at, part in zip(rows_at, parts):
                stats[pl.ds(at + s, 1), :] = jnp.sum(part, axis=0, keepdims=True)

    def tiles(ref, c):
        return [ref[c, :, pair * LANES:(pair + 1) * LANES] for pair in range(bl // 2)]

    mine = [tiles(maps_ref.at[0], c) for c in range(2)]
    shell_sums([32 + 32 * half], [[x * x + y * y for x, y in zip(*mine)]])
    power_copy = pltpu.make_async_remote_copy(
        src_ref=stats.at[own_rows], dst_ref=stats.at[own_rows], send_sem=sent,
        recv_sem=recv_power, device_id={"half": 1 - half}, device_id_type=MESH,
    )
    power_copy.start()
    half_copy.wait_recv()
    theirs = [tiles(other_map, c) for c in range(2)]
    mine = [tiles(maps_ref.at[0], c) for c in range(2)]
    shell_sums([0], [[x * u + y * v for x, y, u, v in zip(*mine, *theirs)]])
    power_copy.wait_recv()
    mine = jnp.sum(stats[...].T, axis=0, keepdims=True)
    total[0] = mine
    stats_in[me] = mine
    for copy in all_to(total, stats_in, recv_stat):
        copy.start()
    whole(stats_in, recv_stat).wait_recv()
    spectra = stats_in[0]
    for n in range(1, N):
        spectra = spectra + stats_in[n]
    spectra_ref[...] = spectra
    rows = sum(sent_rows) + 32 + 2 * (N - 1) + 2 * rl * bl * grid // LANES
    everything = stage_a.at[0, pl.ds(0, rows)]
    pltpu.make_async_remote_copy(
        src_ref=everything, dst_ref=everything, send_sem=sent, recv_sem=recv_half,
        device_id={"half": 1 - half}, device_id_type=MESH,
    ).wait_send()


def finish(shells, maps_in, spectra_ref, counts_ref, maps, power, corr, power_ref, corr_ref, done):
    maps_out = pltpu.make_async_copy(maps_in, maps, done.at[0])
    maps_out.start()
    spectra = spectra_ref[...]
    cross = spectra[:, 0:shells]
    power_first = spectra[:, 32:32 + shells]
    power_second = spectra[:, 64:64 + shells]
    power_ref[0:1, :] = power_first / counts_ref[...]
    power_ref[1:2, :] = power_second / counts_ref[...]
    corr_ref[...] = cross / jnp.sqrt(power_first * power_second + 1e-6)
    small = [
        pltpu.make_async_copy(power_ref, power, done.at[1]),
        pltpu.make_async_copy(corr_ref, corr, done.at[2]),
    ]
    for copy in small:
        copy.start()
    for copy in [maps_out] + small:
        copy.wait()


def solution(mesh):
    R, C = mesh.shape["row"], mesh.shape["col"]
    N = R * C

    def local(particles, orient_bin, tilt_slope, interp_table):
        count, _, grid, plane = particles.shape
        rl, cl, bl = grid // R, plane // C, grid // C
        shells = grid // 2 - 3
        phases = R.bit_length() - 1
        pitch = grid + 8
        bins = interp_table.shape[0]
        steps = C.bit_length() - 1
        nz, n0, n1 = part_rows(rl)
        counts = jnp.asarray(shell_counts(grid)[None], F32)
        vmem, hbm = pl.BlockSpec(memory_space=pltpu.VMEM), pl.BlockSpec(memory_space=pltpu.HBM)
        dma = pltpu.SemaphoreType.DMA
        maps, spectra = pl.pallas_call(
            functools.partial(kernel, (grid, count, R, C, pitch, bins)),
            out_shape=(
                pltpu.VMEM((1, 2, rl, cl), F32),
                pltpu.VMEM((1, LANES), F32),
            ),
            in_specs=[hbm, hbm, hbm, hbm],
            out_specs=(vmem, vmem),
            scratch_shapes=[
                pltpu.VMEM(particles.shape, particles.dtype),
                pltpu.VMEM((bins, grid, grid), interp_table.dtype),
                pltpu.VMEM((bins, 2, grid, grid), interp_table.dtype),
                pltpu.SMEM(orient_bin.shape, jnp.int32),
                pltpu.SMEM(tilt_slope.shape, jnp.int32),
                pltpu.VMEM((count, grid * pitch, LANES), F32),
                pltpu.VMEM((count, C, grid, bl, LANES), F32 if bl % 16 else BF16),
                pltpu.VMEM((C, R, n0 * bl, LANES), F32),
                pltpu.VMEM((C, R, n1 * bl, LANES), F32),
                pltpu.VMEM((C, R, nz * bl, LANES), F32),
                pltpu.VMEM((C, R, n0 * bl, LANES), F32),
                pltpu.VMEM((C, R, n1 * bl, LANES), F32),
                pltpu.VMEM((R, nz * bl, LANES), F32),
                pltpu.VMEM((C, n0 * bl, LANES), F32),
                pltpu.VMEM((C, n1 * bl, LANES), F32),
                pltpu.VMEM((C, R, nz * bl, LANES), F32),
                pltpu.VMEM((2, rl, cl), F32),
                pltpu.VMEM((count * LANES, LANES), BF16),
                pltpu.VMEM((1, 1, LANES), jnp.int32),
                pltpu.VMEM((N, 1, LANES), jnp.int32),
                pltpu.SMEM((N, 1, LANES), jnp.int32),
                pltpu.VMEM((count, R, rl, grid), F32),
                pltpu.VMEM((count, C, bl, grid), F32),
                pltpu.VMEM((C, bl, LANES), F32),
                pltpu.VMEM((bins, rl, grid), F32),
                pltpu.VMEM((bins, bl, LANES), F32),
                pltpu.VMEM((bins, grid, LANES), BF16),
                pltpu.VMEM((rl * bl, LANES), F32),
                pltpu.VMEM((shells, bl // 2, rl, LANES), F32),
                pltpu.VMEM((LANES, LANES), F32),
                pltpu.VMEM((N, 1, LANES), F32),
                pltpu.VMEM((1, 1, LANES), F32),
                dma, dma((phases, 2 * C)), dma((2 * C - 2,)),
                dma((phases,)), dma((C - 1,)),
                dma, dma, dma, dma, dma, dma((count,)), dma, dma, dma, dma,
            ],
            compiler_params=pltpu.CompilerParams(
                collective_id=0, has_side_effects=True, vmem_limit_bytes=VMEM_LIMIT
            ),
        )(orient_bin, tilt_slope, particles, interp_table)
        return pl.pallas_call(
            functools.partial(finish, shells),
            out_shape=(
                jax.ShapeDtypeStruct((1, 2, rl, cl), F32),
                jax.ShapeDtypeStruct((2, shells), F32),
                jax.ShapeDtypeStruct((1, shells), F32),
            ),
            in_specs=[vmem, vmem, vmem],
            out_specs=(hbm, hbm, hbm),
            scratch_shapes=[
                pltpu.VMEM((2, shells), F32), pltpu.VMEM((1, shells), F32), dma((3,)),
            ],
            compiler_params=pltpu.CompilerParams(vmem_limit_bytes=FINISH_LIMIT),
        )(maps, spectra, counts)

    placed = (
        P(("half", "row", "col"), None, None, None),
        P(("half", "row", "col")),
        P(("half", "row", "col"), None),
        P(),
    )
    return jax.shard_map(
        local,
        mesh=mesh,
        in_specs=placed,
        out_specs=(P("half", None, "row", "col"), P(), P("half", None)),
        check_vma=False,
    )
```

```python
import functools

import jax
import jax.numpy as jnp
import numpy as np
from jax import lax
from jax.experimental import pallas as pl
from jax.experimental.pallas import tpu as pltpu
from jax.sharding import PartitionSpec as P

F32 = jnp.float32
BF16 = jnp.bfloat16
LANES = 128
VMEM_LIMIT = 60 * 1024 * 1024
FINISH_LIMIT = 4 * 1024 * 1024
MESH = pl.DeviceIdType.MESH


def dot_nt(left, right):
    return lax.dot_general(left, right, (((1,), (1,)), ((), ())), preferred_element_type=F32)


def dot_nn(left, right):
    return lax.dot_general(left, right, (((1,), (0,)), ((), ())), preferred_element_type=F32)


def block_diagonal(block, copies):
    zero = jnp.zeros_like(block)
    rows = [
        jnp.concatenate([block if i == j else zero for j in range(copies)], axis=1)
        for i in range(copies)
    ]
    return jnp.concatenate(rows, axis=0)


def wedge_mask(limit_same, limit_other, grid, lanes):
    centre = grid // 2
    first = lax.broadcasted_iota(jnp.int32, (grid, lanes), 0) - centre
    third = lax.broadcasted_iota(jnp.int32, (grid, lanes), 1) % grid - centre
    limit = jnp.where(first * third >= 0, limit_same, limit_other)
    inside = 16 * jnp.abs(third) <= limit * jnp.abs(first)
    return jnp.where(inside, 1.0, 0.0).astype(BF16)


def shell_counts(grid):
    centre = grid // 2
    wave = np.arange(grid) - centre
    square = wave * wave
    radius = square[:, None, None] + square[None, :, None] + square[None, None, :]
    shell = np.sum([radius >= k * k for k in range(4, centre)], axis=0)
    return np.bincount(shell[radius < centre * centre], minlength=centre - 3)


def part_rows(rl):
    first = max(1, rl // 4)
    return first, (rl - first) // 2, rl - first - (rl - first) // 2


def plan(R, C, turns, portions):
    phases, steps = R.bit_length() - 1, C.bit_length() - 1
    at = {}
    for n, k in enumerate(turns):
        for g in range(2):
            for phase in range(phases):
                at["row", phase, k, g] = 3.0 + 2.2 * n + 3.5 * phase
    for k in turns:
        if k:
            for g in range(2):
                top = k.bit_length()
                ready = [at["row", phases - 1, k, g]]
                ready += [at["col", k | 1 << m, g] for m in range(top, steps)]
                at["col", k, g] = max(ready) + 3.0
    for k in turns[:-1]:
        top = k.bit_length()
        ready = [at["zcol", k | 1 << m] + 5.2 for m in range(top, steps)]
        at["zcol", k] = max(ready + [4.2 if k == turns[0] else 5.2])
    for phase in range(phases):
        at["zrow", phase] = max(at["zcol", 1 << m] for m in range(steps)) + 2.2 * (phase + 1)
    for core, ahead in enumerate((2, 2)):
        for n, k in enumerate(turns[ahead:]):
            at["send", core, k] = at["row", 0, turns[n], 1] + 0.1 + 0.0 * core
    at["numbers",] = 3.2
    for n in range(portions):
        at["work", n] = 5.0 + 1.1 * n
    return sorted(at, key=at.get)


def kernel(
    dims,
    bins_hbm, tilt_hbm, part_hbm, table_hbm,
    maps_ref, spectra_ref,
    part_ref, first_ref, table_ref, bins_ref, tilt_ref, stage_a, stage_b,
    sums_0, sums_1, sums_z, rows_0, rows_1, rows_z, cols_0, cols_1, cols_z, other_map,
    third_ref, numbers, numbers_in, numbers_s, slab_first, slab_second, wide_second,
    bin_first, bin_second, bin_third, weight,
    inside, stats, stats_in, total,
    sent, recv_row, recv_col, recv_zrow, recv_zcol, recv_num, copy_num,
    recv_stat, recv_half, recv_power, load_part, load_first, load_table, load_bins, load_tilt,
):
    grid, particles, R, C, pitch, bins = dims
    N = R * C
    rl, bl = grid // R, grid // C
    phases, steps = R.bit_length() - 1, C.bit_length() - 1
    half, row, col = lax.axis_index("half"), lax.axis_index("row"), lax.axis_index("col")
    me = row * C + col
    counts = part_rows(rl)
    sums, rows_in, cols_in = (sums_0, sums_1), (rows_0, rows_1), (cols_0, cols_1)

    def peer_id(step):
        peer = (me + step) % N
        return {"row": peer // C, "col": peer % C}

    def flip(index, power):
        return index + (1 - 2 * ((index // power) % 2)) * power

    def power_of(phase, order):
        low, high = 2 ** (phase % phases), 2 ** ((phase + 1) % phases)
        return low + order * (high - low)

    def row_partner(phase, order):
        return {"row": flip(row, power_of(phase, order))}

    def slab_of(index, order):
        slab = row
        for phase in range(phases):
            if (index >> (phases - 1 - phase)) & 1:
                slab = flip(slab, power_of(phase, order))
        return slab

    def col_of(index):
        column = col
        for step in range(steps):
            if (index >> (steps - 1 - step)) & 1:
                column = flip(column, 2 ** step)
        return column

    bins_load = pltpu.make_async_copy(bins_hbm, bins_ref, load_bins)
    tilt_load = pltpu.make_async_copy(tilt_hbm, tilt_ref, load_tilt)
    bins_load.start()
    tilt_load.start()
    first_load = pltpu.make_async_copy(table_hbm.at[:, 0], first_ref, load_first)
    first_load.start()
    part_loads = [
        pltpu.make_async_copy(part_hbm.at[p], part_ref.at[p], load_part.at[p])
        for p in range(particles)
    ]
    for copy in part_loads:
        copy.start()
    table_load = pltpu.make_async_copy(
        table_hbm.at[:, pl.ds(1, 2)], table_ref, load_table
    )
    table_load.start()

    barrier = pltpu.get_barrier_semaphore()
    for step in range(1, N):
        pl.semaphore_signal(barrier, inc=1, device_id=peer_id(step), device_id_type=MESH)
    pl.semaphore_signal(barrier, inc=1, device_id={"half": 1 - half}, device_id_type=MESH)

    bins_load.wait()
    tilt_load.wait()
    lane = lax.broadcasted_iota(jnp.int32, (1, LANES), 1)
    packed = jnp.zeros((1, LANES), jnp.int32)
    for p in range(particles):
        for i, value in enumerate((bins_ref[p], tilt_ref[p, 0], tilt_ref[p, 1])):
            packed = jnp.where(lane == 3 * p + i, value, packed)
    numbers[0] = packed
    numbers_in[me] = packed

    first_load.wait()
    firsts_ = [first_ref[bins_ref[p]] for p in range(particles)]

    def later_tables():
        table_load.wait()
        seconds = []
        for p in range(particles):
            bin_row = bins_ref[p]
            second = table_ref[bin_row, 0].astype(F32)
            for q in range(C):
                slab_second[p, q] = second[q * bl:(q + 1) * bl]
            seconds.append(
                jnp.concatenate([slab_second[p, col_of(k)] for k in range(C)], axis=0).astype(BF16)
            )
            third_ref[p * LANES:(p + 1) * LANES, :] = block_diagonal(table_ref[bin_row, 1].T, 2)
        return seconds

    for copy in part_loads:
        copy.wait()
    low_lanes = lax.broadcasted_iota(jnp.int32, (grid, LANES), 1) < grid
    for p in range(particles):
        first = firsts_[p]
        mask = wedge_mask(tilt_ref[p, 0], tilt_ref[p, 1], grid, LANES)

        for at in range(grid // 2):
            span = slice(at * LANES, (at + 1) * LANES)
            real, imag = part_ref[p, 0, :, span], part_ref[p, 1, :, span]
            crossed = pltpu.roll(jnp.where(low_lanes, imag, real), grid, 1)
            even = jnp.where(low_lanes, real, crossed) * mask
            odd = jnp.where(low_lanes, crossed, imag) * mask
            result = dot_nn(first, jnp.concatenate([even, odd], axis=1))
            for o in range(2):
                to = (2 * at + o) * pitch
                stage_a[p, to:to + grid, :] = result[:, o * LANES:(o + 1) * LANES]

    seconds_ = later_tables()

    def all_to(src, dst, recv):
        return [
            pltpu.make_async_remote_copy(
                src_ref=src.at[0], dst_ref=dst.at[me], send_sem=sent, recv_sem=recv,
                device_id=peer_id(step), device_id_type=MESH,
            )
            for step in range(1, N)
        ]

    def whole(dst, recv):
        return pltpu.make_async_remote_copy(
            src_ref=dst.at[pl.ds(0, N - 1)], dst_ref=dst.at[pl.ds(0, N - 1)],
            send_sem=sent, recv_sem=recv, device_id=peer_id(1), device_id_type=MESH,
        )

    sent_rows = []

    def remote(src, dst, recv, peer, rows):
        copy = pltpu.make_async_remote_copy(
            src_ref=src, dst_ref=dst, send_sem=sent, recv_sem=recv,
            device_id=peer, device_id_type=MESH,
        )
        return copy, rows

    def zcol_copy(k):
        step = steps - k.bit_length()
        return remote(
            sums_z.at[k], cols_z.at[k], recv_zcol.at[k - 1],
            {"col": flip(col, 2 ** step)}, R * counts[0] * bl,
        )

    def zrow_copy(phase):
        keep = R >> (phase + 1)
        span = pl.ds(keep, keep)
        return remote(
            sums_z.at[0, span], rows_z.at[span], recv_zrow.at[phase],
            row_partner(phase, half), keep * counts[0] * bl,
        )

    def row_copy(phase, k, g):
        keep = R >> (phase + 1)
        span = pl.ds(keep, keep)
        return remote(
            sums[g].at[k, span], rows_in[g].at[k, span], recv_row.at[phase, 2 * k + g],
            row_partner(phase, g), keep * counts[1 + g] * bl,
        )

    def col_copy(k, g):
        step = steps - k.bit_length()
        return remote(
            sums[g].at[k, 0], cols_in[g].at[k], recv_col.at[2 * k + g - 2],
            {"col": flip(col, 2 ** step)}, counts[1 + g] * bl,
        )

    def start(message):
        message[0].start()
        sent_rows.append(message[1])

    def start_on(core, k):
        messages = [row_copy(0, k, g) for g in range(2)]
        if core == 0:
            sent_rows.extend(rows for _, rows in messages)

        @pl.when(half == core)
        def _():
            for copy, _ in messages:
                copy.start()

    firsts_of = [0, R * counts[0], R * (counts[0] + counts[1])]
    within = [0, counts[0], counts[0] + counts[1]]

    def along_second(parts):
        places = [
            (firsts_of[g] + j * counts[g] + i, slab_of(j, order) * rl + within[g] + i)
            for g, order, j0, j1 in parts
            for j in range(j0, j1)
            for i in range(counts[g])
        ]
        for n in range(0, len(places), 2):
            pair = places[n:n + 2]
            for p in range(particles):
                block = jnp.concatenate(
                    [stage_a[p, pl.ds(a, grid, stride=pitch), :] for _, a in pair], axis=1
                ).astype(BF16)
                result = dot_nn(seconds_[p], block).astype(stage_b.dtype)
                for i, (to, _) in enumerate(pair):
                    for k in range(C):
                        stage_b[p, k, to] = result[
                            k * bl:(k + 1) * bl, i * LANES:(i + 1) * LANES
                        ]

    def along_third(parts):
        pieces, places = [], []
        for to, k, g, j0, j1 in parts:
            rows = counts[g] * bl
            low, high = (firsts_of[g] + j * counts[g] for j in (j0, j1))
            pieces.append(jnp.concatenate(
                [
                    stage_b[p, k, low:high].reshape((high - low) * bl, LANES)
                    for p in range(particles)
                ],
                axis=1,
            ))
            places += [(to, k, j, rows) for j in range(j0, j1)]
        result = dot_nn(jnp.concatenate(pieces, axis=0).astype(BF16), third_ref[...])
        at = 0
        for to, k, j, rows in places:
            to[k, j] = result[at:at + rows]
            at += rows

    def row_parts(turn, j0, j1):
        return [(sums[g], k, 1 + g, j0, j1) for k in turn for g in range(2)]

    turns = sorted(
        range(C), key=lambda k: -sum(((k >> i) & 1) << (steps - 1 - i) for i in range(steps))
    )
    along_second([(1 + g, g, R // 2, R) for g in range(2)] + [(0, half, 0, R)])
    along_third(row_parts(turns[:1], R // 2, R) + [(sums_z, k, 0, 0, R) for k in range(C // 2, C)])
    pl.semaphore_wait(barrier, N)
    for copy in all_to(numbers, numbers_in, recv_num):
        copy.start()
    for g in range(2):
        start(row_copy(0, turns[0], g))
    for k in [k for k in turns if k >= C // 2]:
        start(zcol_copy(k))
    along_third(row_parts(turns[1:], R // 2, R))
    start_on(0, turns[1])
    start_on(1, turns[1])
    along_second([(1 + g, g, 0, R // 2) for g in range(2)])
    along_third(row_parts(turns, 0, R // 2) + [(sums_z, k, 0, 0, R) for k in range(C // 2)])

    local = pltpu.make_async_copy(numbers_in, numbers_s, copy_num)
    weight[...] = jnp.zeros_like(weight)
    ones = jnp.ones((grid, LANES), BF16)

    def bin_tables(n, carry):
        first = first_ref[n].astype(F32)
        second = dot_nn(table_ref[n, 0], ones)
        for r in range(R):
            slab_first[0, r] = first[r * rl:(r + 1) * rl]
        for q in range(C):
            wide_second[q] = second[q * bl:(q + 1) * bl]
        bin_first[n] = slab_first[0, row]
        bin_second[n] = wide_second[col]
        across = table_ref[n, 1].T
        bin_third[n] = jnp.concatenate([across, across], axis=1)
        return carry

    lax.fori_loop(0, bins, bin_tables, 0, unroll=4)

    together = 2
    first_wave = lax.broadcasted_iota(jnp.int32, (grid, LANES), 0) - grid // 2
    third_wave = lax.broadcasted_iota(jnp.int32, (grid, LANES), 1) % grid - grid // 2
    same_side = first_wave * third_wave >= 0
    first_size, third_size = jnp.abs(first_wave), 16 * jnp.abs(third_wave)
    low_rows = lax.broadcasted_iota(jnp.int32, (rl, LANES), 1) < grid
    low_seconds = lax.broadcasted_iota(jnp.int32, (bl, LANES), 1) < grid

    def add_weight(step, carry):
        members = [(step * together + n, p) for n in range(together) for p in range(particles)]
        blocks, thirds = [], []
        for i in range(0, len(members), 2):
            numbers_of = [
                [numbers_s[n, 0, 3 * p + v] for v in range(3)] for n, p in members[i:i + 2]
            ]
            limit = jnp.where(
                same_side,
                jnp.where(low_lanes, numbers_of[0][1], numbers_of[1][1]),
                jnp.where(low_lanes, numbers_of[0][2], numbers_of[1][2]),
            )
            mask = jnp.where(third_size <= limit * first_size, 1.0, 0.0).astype(BF16)
            along = [dot_nn(bin_first[value[0]].astype(BF16), mask) for value in numbers_of]
            first = jnp.where(low_rows, along[0], along[1]).astype(BF16).astype(F32)
            second = jnp.where(
                low_seconds, bin_second[numbers_of[0][0]], bin_second[numbers_of[1][0]]
            )
            blocks.append(
                jnp.concatenate([first[a:a + 1] * second for a in range(rl)], axis=0).astype(BF16)
            )
            thirds += [bin_third[value[0]] for value in numbers_of]
        weight[...] += dot_nn(jnp.concatenate(blocks, axis=1), jnp.concatenate(thirds, axis=0))
        return carry

    centre = grid // 2
    shells = centre - 3
    tile_rows = lax.broadcasted_iota(jnp.int32, (rl, LANES), 0)
    tile_lanes = lax.broadcasted_iota(jnp.int32, (rl, LANES), 1)
    wave_first = row * rl + tile_rows - centre
    wave_third = tile_lanes % grid - centre
    fixed = wave_first * wave_first + wave_third * wave_third
    radius = []
    for pair in range(bl // 2):
        wave_second = col * bl + 2 * pair + tile_lanes // grid - centre
        radius.append(fixed + wave_second * wave_second)
    for s in range(shells):
        least = (s + 3) * (s + 3) if s else 0
        beyond = (s + 4) * (s + 4)
        for pair, r2 in enumerate(radius):
            inside[s, pair] = jnp.where((r2 >= least) & (r2 < beyond), 1.0, 0.0)

    groups = N // together
    portions = 8
    done = set()
    worked = [0]

    def work():
        n = worked[0]
        worked[0] = n + 1
        if n == 0:
            local.wait()
        low, high = groups * n // portions, groups * (n + 1) // portions
        if high > low:
            lax.fori_loop(low, high, add_weight, 0)

    def col_ready(k, g):
        top = k.bit_length()
        return all(("row", phases - 1, k, g) in done and ("col", k | 1 << m, g) in done for m in range(top, steps)) and ("row", phases - 1, k, g) in done

    def maybe_col(k, g):
        if k and col_ready(k, g) and ("sentcol", k, g) not in done:
            done.add(("sentcol", k, g))
            start(col_copy(k, g))

    def take(event):
        kind = event[0]
        if kind == "work":
            work()
            return
        if kind == "send":
            start_on(*event[1:])
            return
        if kind == "numbers":
            whole(numbers_in, recv_num).wait_recv()
            local.start()
            return
        if kind == "zcol":
            zcol_copy(event[1])[0].wait_recv()
        elif kind == "zrow":
            zrow_copy(event[1])[0].wait_recv()
        elif kind == "row":
            row_copy(*event[1:])[0].wait_recv()
        else:
            col_copy(*event[1:])[0].wait_recv()
        done.add(event)
        if kind == "zcol":
            k = event[1]
            into = k - (1 << k.bit_length() - 1)
            sums_z[into] = sums_z[into] + cols_z[k]
            if all(("zcol", into | 1 << m) in done for m in range(into.bit_length(), steps)):
                start(zcol_copy(into) if into else zrow_copy(0))
        elif kind == "zrow":
            phase = event[1]
            keep = R >> (phase + 1)
            sums_z[0, :keep] = sums_z[0, :keep] + rows_z[keep:2 * keep]
            if phase + 1 < phases:
                start(zrow_copy(phase + 1))
        elif kind == "row":
            _, phase, k, g = event
            keep = R >> (phase + 1)
            sums[g][k, :keep] = sums[g][k, :keep] + rows_in[g][k, keep:2 * keep]
            if phase + 1 < phases:
                start(row_copy(phase + 1, k, g))
            else:
                maybe_col(k, g)
        else:
            _, k, g = event
            into = k - (1 << k.bit_length() - 1)
            sums[g][into, 0] = sums[g][into, 0] + cols_in[g][k]
            maybe_col(into, g)

    for event in plan(R, C, turns, portions):
        take(event)

    block = jnp.concatenate([sums_z[0, 0], sums_0[0, 0], sums_1[0, 0]], axis=0)
    weight[...] = block / (weight[...] + 1.0)
    low = lax.broadcasted_iota(jnp.int32, (rl, LANES), 1) < grid
    for pair in range(bl // 2):
        span = slice(pair * LANES, (pair + 1) * LANES)
        even, odd = (weight[pl.ds(2 * pair + i, rl, stride=bl), :] for i in range(2))
        maps_ref[0, 0, :, span] = jnp.where(low, even, pltpu.roll(odd, grid, 1))
        maps_ref[0, 1, :, span] = jnp.where(low, pltpu.roll(even, grid, 1), odd)

    half_copy = pltpu.make_async_remote_copy(
        src_ref=maps_ref.at[0], dst_ref=other_map, send_sem=sent, recv_sem=recv_half,
        device_id={"half": 1 - half}, device_id_type=MESH,
    )
    half_copy.start()
    own_rows = pl.ds(pl.multiple_of(32 + 32 * half, 32), 32)
    for rows in (pl.ds(0, 32), own_rows, pl.ds(96, 32)):
        stats[rows] = jnp.zeros((32, LANES), F32)

    def shell_sums(rows_at, values):
        for s in range(shells):
            parts = [jnp.zeros((rl, LANES), F32) for _ in values]
            for pair in range(bl // 2):
                mask = inside[s, pair]
                parts = [part + mask * value[pair] for part, value in zip(parts, values)]
            for at, part in zip(rows_at, parts):
                stats[pl.ds(at + s, 1), :] = jnp.sum(part, axis=0, keepdims=True)

    def tiles(ref, c):
        return [ref[c, :, pair * LANES:(pair + 1) * LANES] for pair in range(bl // 2)]

    mine = [tiles(maps_ref.at[0], c) for c in range(2)]
    shell_sums([32 + 32 * half], [[x * x + y * y for x, y in zip(*mine)]])
    power_copy = pltpu.make_async_remote_copy(
        src_ref=stats.at[own_rows], dst_ref=stats.at[own_rows], send_sem=sent,
        recv_sem=recv_power, device_id={"half": 1 - half}, device_id_type=MESH,
    )
    power_copy.start()
    half_copy.wait_recv()
    theirs = [tiles(other_map, c) for c in range(2)]
    mine = [tiles(maps_ref.at[0], c) for c in range(2)]
    shell_sums([0], [[x * u + y * v for x, y, u, v in zip(*mine, *theirs)]])
    power_copy.wait_recv()
    mine = jnp.sum(stats[...].T, axis=0, keepdims=True)
    total[0] = mine
    stats_in[me] = mine
    for copy in all_to(total, stats_in, recv_stat):
        copy.start()
    whole(stats_in, recv_stat).wait_recv()
    spectra = stats_in[0]
    for n in range(1, N):
        spectra = spectra + stats_in[n]
    spectra_ref[...] = spectra
    rows = sum(sent_rows) + 32 + 2 * (N - 1) + 2 * rl * bl * grid // LANES
    everything = stage_a.at[0, pl.ds(0, rows)]
    pltpu.make_async_remote_copy(
        src_ref=everything, dst_ref=everything, send_sem=sent, recv_sem=recv_half,
        device_id={"half": 1 - half}, device_id_type=MESH,
    ).wait_send()


def finish(shells, maps_in, spectra_ref, counts_ref, maps, power, corr, power_ref, corr_ref, done):
    maps_out = pltpu.make_async_copy(maps_in, maps, done.at[0])
    maps_out.start()
    spectra = spectra_ref[...]
    cross = spectra[:, 0:shells]
    power_first = spectra[:, 32:32 + shells]
    power_second = spectra[:, 64:64 + shells]
    power_ref[0:1, :] = power_first / counts_ref[...]
    power_ref[1:2, :] = power_second / counts_ref[...]
    corr_ref[...] = cross / jnp.sqrt(power_first * power_second + 1e-6)
    small = [
        pltpu.make_async_copy(power_ref, power, done.at[1]),
        pltpu.make_async_copy(corr_ref, corr, done.at[2]),
    ]
    for copy in small:
        copy.start()
    for copy in [maps_out] + small:
        copy.wait()


def solution(mesh):
    R, C = mesh.shape["row"], mesh.shape["col"]
    N = R * C

    def local(particles, orient_bin, tilt_slope, interp_table):
        count, _, grid, plane = particles.shape
        rl, cl, bl = grid // R, plane // C, grid // C
        shells = grid // 2 - 3
        phases = R.bit_length() - 1
        pitch = grid + 8
        bins = interp_table.shape[0]
        steps = C.bit_length() - 1
        nz, n0, n1 = part_rows(rl)
        counts = jnp.asarray(shell_counts(grid)[None], F32)
        vmem, hbm = pl.BlockSpec(memory_space=pltpu.VMEM), pl.BlockSpec(memory_space=pltpu.HBM)
        dma = pltpu.SemaphoreType.DMA
        maps, spectra = pl.pallas_call(
            functools.partial(kernel, (grid, count, R, C, pitch, bins)),
            out_shape=(
                pltpu.VMEM((1, 2, rl, cl), F32),
                pltpu.VMEM((1, LANES), F32),
            ),
            in_specs=[hbm, hbm, hbm, hbm],
            out_specs=(vmem, vmem),
            scratch_shapes=[
                pltpu.VMEM(particles.shape, particles.dtype),
                pltpu.VMEM((bins, grid, grid), interp_table.dtype),
                pltpu.VMEM((bins, 2, grid, grid), interp_table.dtype),
                pltpu.SMEM(orient_bin.shape, jnp.int32),
                pltpu.SMEM(tilt_slope.shape, jnp.int32),
                pltpu.VMEM((count, grid * pitch, LANES), F32),
                pltpu.VMEM((count, C, grid, bl, LANES), F32 if bl % 16 else BF16),
                pltpu.VMEM((C, R, n0 * bl, LANES), F32),
                pltpu.VMEM((C, R, n1 * bl, LANES), F32),
                pltpu.VMEM((C, R, nz * bl, LANES), F32),
                pltpu.VMEM((C, R, n0 * bl, LANES), F32),
                pltpu.VMEM((C, R, n1 * bl, LANES), F32),
                pltpu.VMEM((R, nz * bl, LANES), F32),
                pltpu.VMEM((C, n0 * bl, LANES), F32),
                pltpu.VMEM((C, n1 * bl, LANES), F32),
                pltpu.VMEM((C, R, nz * bl, LANES), F32),
                pltpu.VMEM((2, rl, cl), F32),
                pltpu.VMEM((count * LANES, LANES), BF16),
                pltpu.VMEM((1, 1, LANES), jnp.int32),
                pltpu.VMEM((N, 1, LANES), jnp.int32),
                pltpu.SMEM((N, 1, LANES), jnp.int32),
                pltpu.VMEM((count, R, rl, grid), F32),
                pltpu.VMEM((count, C, bl, grid), F32),
                pltpu.VMEM((C, bl, LANES), F32),
                pltpu.VMEM((bins, rl, grid), F32),
                pltpu.VMEM((bins, bl, LANES), F32),
                pltpu.VMEM((bins, grid, LANES), BF16),
                pltpu.VMEM((rl * bl, LANES), F32),
                pltpu.VMEM((shells, bl // 2, rl, LANES), F32),
                pltpu.VMEM((LANES, LANES), F32),
                pltpu.VMEM((N, 1, LANES), F32),
                pltpu.VMEM((1, 1, LANES), F32),
                dma, dma((phases, 2 * C)), dma((2 * C - 2,)),
                dma((phases,)), dma((C - 1,)),
                dma, dma, dma, dma, dma, dma((count,)), dma, dma, dma, dma,
            ],
            compiler_params=pltpu.CompilerParams(
                collective_id=0, has_side_effects=True, vmem_limit_bytes=VMEM_LIMIT
            ),
        )(orient_bin, tilt_slope, particles, interp_table)
        return pl.pallas_call(
            functools.partial(finish, shells),
            out_shape=(
                jax.ShapeDtypeStruct((1, 2, rl, cl), F32),
                jax.ShapeDtypeStruct((2, shells), F32),
                jax.ShapeDtypeStruct((1, shells), F32),
            ),
            in_specs=[vmem, vmem, vmem],
            out_specs=(hbm, hbm, hbm),
            scratch_shapes=[
                pltpu.VMEM((2, shells), F32), pltpu.VMEM((1, shells), F32), dma((3,)),
            ],
            compiler_params=pltpu.CompilerParams(vmem_limit_bytes=FINISH_LIMIT),
        )(maps, spectra, counts)

    placed = (
        P(("half", "row", "col"), None, None, None),
        P(("half", "row", "col")),
        P(("half", "row", "col"), None),
        P(),
    )
    return jax.shard_map(
        local,
        mesh=mesh,
        in_specs=placed,
        out_specs=(P("half", None, "row", "col"), P(), P("half", None)),
        check_vma=False,
    )
```

```python
import functools

import jax
import jax.numpy as jnp
import numpy as np
from jax import lax
from jax.experimental import pallas as pl
from jax.experimental.pallas import tpu as pltpu
from jax.sharding import PartitionSpec as P

F32 = jnp.float32
BF16 = jnp.bfloat16
LANES = 128
VMEM_LIMIT = 60 * 1024 * 1024
FINISH_LIMIT = 4 * 1024 * 1024
MESH = pl.DeviceIdType.MESH


def dot_nt(left, right):
    return lax.dot_general(left, right, (((1,), (1,)), ((), ())), preferred_element_type=F32)


def dot_nn(left, right):
    return lax.dot_general(left, right, (((1,), (0,)), ((), ())), preferred_element_type=F32)


def block_diagonal(block, copies):
    zero = jnp.zeros_like(block)
    rows = [
        jnp.concatenate([block if i == j else zero for j in range(copies)], axis=1)
        for i in range(copies)
    ]
    return jnp.concatenate(rows, axis=0)


def wedge_mask(limit_same, limit_other, grid, lanes):
    centre = grid // 2
    first = lax.broadcasted_iota(jnp.int32, (grid, lanes), 0) - centre
    third = lax.broadcasted_iota(jnp.int32, (grid, lanes), 1) % grid - centre
    limit = jnp.where(first * third >= 0, limit_same, limit_other)
    inside = 16 * jnp.abs(third) <= limit * jnp.abs(first)
    return jnp.where(inside, 1.0, 0.0).astype(BF16)


def shell_counts(grid):
    centre = grid // 2
    wave = np.arange(grid) - centre
    square = wave * wave
    radius = square[:, None, None] + square[None, :, None] + square[None, None, :]
    shell = np.sum([radius >= k * k for k in range(4, centre)], axis=0)
    return np.bincount(shell[radius < centre * centre], minlength=centre - 3)


def part_rows(rl):
    first = max(1, rl // 4)
    return first, (rl - first) // 2, rl - first - (rl - first) // 2


def plan(R, C, turns, portions):
    phases, steps = R.bit_length() - 1, C.bit_length() - 1
    at = {}
    for n, k in enumerate(turns):
        for g in range(2):
            for phase in range(phases):
                at["row", phase, k, g] = 3.0 + 2.2 * n + 3.5 * phase
    for k in turns:
        if k:
            for g in range(2):
                top = k.bit_length()
                ready = [at["row", phases - 1, k, g]]
                ready += [at["col", k | 1 << m, g] for m in range(top, steps)]
                at["col", k, g] = max(ready) + 3.0
    for k in turns[:-1]:
        top = k.bit_length()
        ready = [at["zcol", k | 1 << m] + 5.2 for m in range(top, steps)]
        at["zcol", k] = max(ready + [4.2 if k == turns[0] else 5.2])
    for phase in range(phases):
        at["zrow", phase] = max(at["zcol", 1 << m] for m in range(steps)) + 2.2 * (phase + 1)
    for core, ahead in enumerate((2, 2)):
        for n, k in enumerate(turns[ahead:]):
            at["send", core, k] = at["row", 0, turns[n], 1] + 0.1 + 0.0 * core
    at["numbers",] = 3.2
    for n in range(portions):
        at["work", n] = 5.0 + 1.1 * n
    return sorted(at, key=at.get)


def kernel(
    dims,
    bins_hbm, tilt_hbm, part_hbm, table_hbm,
    maps_ref, spectra_ref,
    part_ref, first_ref, table_ref, bins_ref, tilt_ref, stage_a, stage_b,
    sums_0, sums_1, sums_z, rows_0, rows_1, rows_z, cols_0, cols_1, cols_z, other_map,
    third_ref, numbers, numbers_in, numbers_s, slab_first, slab_second, wide_second,
    bin_first, bin_second, bin_third, weight,
    inside, stats, stats_in, total,
    sent, recv_row, recv_col, recv_zrow, recv_zcol, recv_num, copy_num,
    recv_stat, recv_half, recv_power, load_part, load_first, load_table, load_bins, load_tilt,
):
    grid, particles, R, C, pitch, bins = dims
    N = R * C
    rl, bl = grid // R, grid // C
    phases, steps = R.bit_length() - 1, C.bit_length() - 1
    half, row, col = lax.axis_index("half"), lax.axis_index("row"), lax.axis_index("col")
    me = row * C + col
    counts = part_rows(rl)
    sums, rows_in, cols_in = (sums_0, sums_1), (rows_0, rows_1), (cols_0, cols_1)

    def peer_id(step):
        peer = (me + step) % N
        return {"row": peer // C, "col": peer % C}

    def flip(index, power):
        return index + (1 - 2 * ((index // power) % 2)) * power

    def power_of(phase, order):
        low, high = 2 ** (phase % phases), 2 ** ((phase + 1) % phases)
        return low + order * (high - low)

    def row_partner(phase, order):
        return {"row": flip(row, power_of(phase, order))}

    def slab_of(index, order):
        slab = row
        for phase in range(phases):
            if (index >> (phases - 1 - phase)) & 1:
                slab = flip(slab, power_of(phase, order))
        return slab

    def col_of(index):
        column = col
        for step in range(steps):
            if (index >> (steps - 1 - step)) & 1:
                column = flip(column, 2 ** step)
        return column

    bins_load = pltpu.make_async_copy(bins_hbm, bins_ref, load_bins)
    tilt_load = pltpu.make_async_copy(tilt_hbm, tilt_ref, load_tilt)
    bins_load.start()
    tilt_load.start()
    first_load = pltpu.make_async_copy(table_hbm.at[:, 0], first_ref, load_first)
    first_load.start()
    part_loads = [
        pltpu.make_async_copy(part_hbm.at[p], part_ref.at[p], load_part.at[p])
        for p in range(particles)
    ]
    for copy in part_loads:
        copy.start()
    table_load = pltpu.make_async_copy(
        table_hbm.at[:, pl.ds(1, 2)], table_ref, load_table
    )
    table_load.start()

    barrier = pltpu.get_barrier_semaphore()
    for step in range(1, N):
        pl.semaphore_signal(barrier, inc=1, device_id=peer_id(step), device_id_type=MESH)
    pl.semaphore_signal(barrier, inc=1, device_id={"half": 1 - half}, device_id_type=MESH)

    bins_load.wait()
    tilt_load.wait()
    lane = lax.broadcasted_iota(jnp.int32, (1, LANES), 1)
    packed = jnp.zeros((1, LANES), jnp.int32)
    for p in range(particles):
        for i, value in enumerate((bins_ref[p], tilt_ref[p, 0], tilt_ref[p, 1])):
            packed = jnp.where(lane == 3 * p + i, value, packed)
    numbers[0] = packed
    numbers_in[me] = packed

    first_load.wait()
    firsts_ = [first_ref[bins_ref[p]] for p in range(particles)]

    def later_tables():
        table_load.wait()
        seconds = []
        for p in range(particles):
            bin_row = bins_ref[p]
            second = table_ref[bin_row, 0].astype(F32)
            for q in range(C):
                slab_second[p, q] = second[q * bl:(q + 1) * bl]
            seconds.append(
                jnp.concatenate([slab_second[p, col_of(k)] for k in range(C)], axis=0).astype(BF16)
            )
            third_ref[p * LANES:(p + 1) * LANES, :] = block_diagonal(table_ref[bin_row, 1].T, 2)
        return seconds

    for copy in part_loads:
        copy.wait()
    seconds_ = later_tables()
    low_lanes = lax.broadcasted_iota(jnp.int32, (grid, LANES), 1) < grid
    for p in range(particles):
        first = firsts_[p]
        mask = wedge_mask(tilt_ref[p, 0], tilt_ref[p, 1], grid, LANES)

        for at in range(grid // 2):
            span = slice(at * LANES, (at + 1) * LANES)
            real, imag = part_ref[p, 0, :, span], part_ref[p, 1, :, span]
            crossed = pltpu.roll(jnp.where(low_lanes, imag, real), grid, 1)
            even = jnp.where(low_lanes, real, crossed) * mask
            odd = jnp.where(low_lanes, crossed, imag) * mask
            result = dot_nn(first, jnp.concatenate([even, odd], axis=1))
            for o in range(2):
                to = (2 * at + o) * pitch
                stage_a[p, to:to + grid, :] = result[:, o * LANES:(o + 1) * LANES]

    def all_to(src, dst, recv):
        return [
            pltpu.make_async_remote_copy(
                src_ref=src.at[0], dst_ref=dst.at[me], send_sem=sent, recv_sem=recv,
                device_id=peer_id(step), device_id_type=MESH,
            )
            for step in range(1, N)
        ]

    def whole(dst, recv):
        return pltpu.make_async_remote_copy(
            src_ref=dst.at[pl.ds(0, N - 1)], dst_ref=dst.at[pl.ds(0, N - 1)],
            send_sem=sent, recv_sem=recv, device_id=peer_id(1), device_id_type=MESH,
        )

    sent_rows = []

    def remote(src, dst, recv, peer, rows):
        copy = pltpu.make_async_remote_copy(
            src_ref=src, dst_ref=dst, send_sem=sent, recv_sem=recv,
            device_id=peer, device_id_type=MESH,
        )
        return copy, rows

    def zcol_copy(k):
        step = steps - k.bit_length()
        return remote(
            sums_z.at[k], cols_z.at[k], recv_zcol.at[k - 1],
            {"col": flip(col, 2 ** step)}, R * counts[0] * bl,
        )

    def zrow_copy(phase):
        keep = R >> (phase + 1)
        span = pl.ds(keep, keep)
        return remote(
            sums_z.at[0, span], rows_z.at[span], recv_zrow.at[phase],
            row_partner(phase, half), keep * counts[0] * bl,
        )

    def row_copy(phase, k, g):
        keep = R >> (phase + 1)
        span = pl.ds(keep, keep)
        return remote(
            sums[g].at[k, span], rows_in[g].at[k, span], recv_row.at[phase, 2 * k + g],
            row_partner(phase, g), keep * counts[1 + g] * bl,
        )

    def col_copy(k, g):
        step = steps - k.bit_length()
        return remote(
            sums[g].at[k, 0], cols_in[g].at[k], recv_col.at[2 * k + g - 2],
            {"col": flip(col, 2 ** step)}, counts[1 + g] * bl,
        )

    def start(message):
        message[0].start()
        sent_rows.append(message[1])

    def start_on(core, k):
        messages = [row_copy(0, k, g) for g in range(2)]
        if core == 0:
            sent_rows.extend(rows for _, rows in messages)

        @pl.when(half == core)
        def _():
            for copy, _ in messages:
                copy.start()

    firsts_of = [0, R * counts[0], R * (counts[0] + counts[1])]
    within = [0, counts[0], counts[0] + counts[1]]

    def along_second(parts):
        places = [
            (firsts_of[g] + j * counts[g] + i, slab_of(j, order) * rl + within[g] + i)
            for g, order, j0, j1 in parts
            for j in range(j0, j1)
            for i in range(counts[g])
        ]
        for n in range(0, len(places), 2):
            pair = places[n:n + 2]
            for p in range(particles):
                block = jnp.concatenate(
                    [stage_a[p, pl.ds(a, grid, stride=pitch), :] for _, a in pair], axis=1
                ).astype(BF16)
                result = dot_nn(seconds_[p], block).astype(stage_b.dtype)
                for i, (to, _) in enumerate(pair):
                    for k in range(C):
                        stage_b[p, k, to] = result[
                            k * bl:(k + 1) * bl, i * LANES:(i + 1) * LANES
                        ]

    def along_third(parts):
        pieces, places = [], []
        for to, k, g, j0, j1 in parts:
            rows = counts[g] * bl
            low, high = (firsts_of[g] + j * counts[g] for j in (j0, j1))
            pieces.append(jnp.concatenate(
                [
                    stage_b[p, k, low:high].reshape((high - low) * bl, LANES)
                    for p in range(particles)
                ],
                axis=1,
            ))
            places += [(to, k, j, rows) for j in range(j0, j1)]
        result = dot_nn(jnp.concatenate(pieces, axis=0).astype(BF16), third_ref[...])
        at = 0
        for to, k, j, rows in places:
            to[k, j] = result[at:at + rows]
            at += rows

    def row_parts(turn, j0, j1):
        return [(sums[g], k, 1 + g, j0, j1) for k in turn for g in range(2)]

    turns = sorted(
        range(C), key=lambda k: -sum(((k >> i) & 1) << (steps - 1 - i) for i in range(steps))
    )
    along_second([(1 + g, g, R // 2, R) for g in range(2)] + [(0, half, 0, R)])
    along_third(row_parts(turns[:1], R // 2, R) + [(sums_z, k, 0, 0, R) for k in range(C // 2, C)])
    pl.semaphore_wait(barrier, N)
    for copy in all_to(numbers, numbers_in, recv_num):
        copy.start()
    for g in range(2):
        start(row_copy(0, turns[0], g))
    for k in [k for k in turns if k >= C // 2]:
        start(zcol_copy(k))
    along_third(row_parts(turns[1:], R // 2, R))
    start_on(0, turns[1])
    start_on(1, turns[1])
    along_second([(1 + g, g, 0, R // 2) for g in range(2)])
    along_third(row_parts(turns, 0, R // 2) + [(sums_z, k, 0, 0, R) for k in range(C // 2)])

    local = pltpu.make_async_copy(numbers_in, numbers_s, copy_num)
    weight[...] = jnp.zeros_like(weight)
    ones = jnp.ones((grid, LANES), BF16)

    def bin_tables(n, carry):
        first = first_ref[n].astype(F32)
        second = dot_nn(table_ref[n, 0], ones)
        for r in range(R):
            slab_first[0, r] = first[r * rl:(r + 1) * rl]
        for q in range(C):
            wide_second[q] = second[q * bl:(q + 1) * bl]
        bin_first[n] = slab_first[0, row]
        bin_second[n] = wide_second[col]
        across = table_ref[n, 1].T
        bin_third[n] = jnp.concatenate([across, across], axis=1)
        return carry

    lax.fori_loop(0, bins, bin_tables, 0, unroll=4)

    together = 2
    first_wave = lax.broadcasted_iota(jnp.int32, (grid, LANES), 0) - grid // 2
    third_wave = lax.broadcasted_iota(jnp.int32, (grid, LANES), 1) % grid - grid // 2
    same_side = first_wave * third_wave >= 0
    first_size, third_size = jnp.abs(first_wave), 16 * jnp.abs(third_wave)
    low_rows = lax.broadcasted_iota(jnp.int32, (rl, LANES), 1) < grid
    low_seconds = lax.broadcasted_iota(jnp.int32, (bl, LANES), 1) < grid

    def add_weight(step, carry):
        members = [(step * together + n, p) for n in range(together) for p in range(particles)]
        blocks, thirds = [], []
        for i in range(0, len(members), 2):
            numbers_of = [
                [numbers_s[n, 0, 3 * p + v] for v in range(3)] for n, p in members[i:i + 2]
            ]
            limit = jnp.where(
                same_side,
                jnp.where(low_lanes, numbers_of[0][1], numbers_of[1][1]),
                jnp.where(low_lanes, numbers_of[0][2], numbers_of[1][2]),
            )
            mask = jnp.where(third_size <= limit * first_size, 1.0, 0.0).astype(BF16)
            along = [dot_nn(bin_first[value[0]].astype(BF16), mask) for value in numbers_of]
            first = jnp.where(low_rows, along[0], along[1]).astype(BF16).astype(F32)
            second = jnp.where(
                low_seconds, bin_second[numbers_of[0][0]], bin_second[numbers_of[1][0]]
            )
            blocks.append(
                jnp.concatenate([first[a:a + 1] * second for a in range(rl)], axis=0).astype(BF16)
            )
            thirds += [bin_third[value[0]] for value in numbers_of]
        weight[...] += dot_nn(jnp.concatenate(blocks, axis=1), jnp.concatenate(thirds, axis=0))
        return carry

    centre = grid // 2
    shells = centre - 3
    tile_rows = lax.broadcasted_iota(jnp.int32, (rl, LANES), 0)
    tile_lanes = lax.broadcasted_iota(jnp.int32, (rl, LANES), 1)
    wave_first = row * rl + tile_rows - centre
    wave_third = tile_lanes % grid - centre
    fixed = wave_first * wave_first + wave_third * wave_third
    radius = []
    for pair in range(bl // 2):
        wave_second = col * bl + 2 * pair + tile_lanes // grid - centre
        radius.append(fixed + wave_second * wave_second)
    for s in range(shells):
        least = (s + 3) * (s + 3) if s else 0
        beyond = (s + 4) * (s + 4)
        for pair, r2 in enumerate(radius):
            inside[s, pair] = jnp.where((r2 >= least) & (r2 < beyond), 1.0, 0.0)

    groups = N // together
    portions = 8
    done = set()
    worked = [0]

    def work():
        n = worked[0]
        worked[0] = n + 1
        if n == 0:
            local.wait()
        low, high = groups * n // portions, groups * (n + 1) // portions
        if high > low:
            lax.fori_loop(low, high, add_weight, 0)

    def col_ready(k, g):
        top = k.bit_length()
        return all(("row", phases - 1, k, g) in done and ("col", k | 1 << m, g) in done for m in range(top, steps)) and ("row", phases - 1, k, g) in done

    def maybe_col(k, g):
        if k and col_ready(k, g) and ("sentcol", k, g) not in done:
            done.add(("sentcol", k, g))
            start(col_copy(k, g))

    def take(event):
        kind = event[0]
        if kind == "work":
            work()
            return
        if kind == "send":
            start_on(*event[1:])
            return
        if kind == "numbers":
            whole(numbers_in, recv_num).wait_recv()
            local.start()
            return
        if kind == "zcol":
            zcol_copy(event[1])[0].wait_recv()
        elif kind == "zrow":
            zrow_copy(event[1])[0].wait_recv()
        elif kind == "row":
            row_copy(*event[1:])[0].wait_recv()
        else:
            col_copy(*event[1:])[0].wait_recv()
        done.add(event)
        if kind == "zcol":
            k = event[1]
            into = k - (1 << k.bit_length() - 1)
            sums_z[into] = sums_z[into] + cols_z[k]
            if all(("zcol", into | 1 << m) in done for m in range(into.bit_length(), steps)):
                start(zcol_copy(into) if into else zrow_copy(0))
        elif kind == "zrow":
            phase = event[1]
            keep = R >> (phase + 1)
            sums_z[0, :keep] = sums_z[0, :keep] + rows_z[keep:2 * keep]
            if phase + 1 < phases:
                start(zrow_copy(phase + 1))
        elif kind == "row":
            _, phase, k, g = event
            keep = R >> (phase + 1)
            sums[g][k, :keep] = sums[g][k, :keep] + rows_in[g][k, keep:2 * keep]
            if phase + 1 < phases:
                start(row_copy(phase + 1, k, g))
            else:
                maybe_col(k, g)
        else:
            _, k, g = event
            into = k - (1 << k.bit_length() - 1)
            sums[g][into, 0] = sums[g][into, 0] + cols_in[g][k]
            maybe_col(into, g)

    for event in plan(R, C, turns, portions):
        take(event)

    block = jnp.concatenate([sums_z[0, 0], sums_0[0, 0], sums_1[0, 0]], axis=0)
    weight[...] = block / (weight[...] + 1.0)
    low = lax.broadcasted_iota(jnp.int32, (rl, LANES), 1) < grid
    for pair in range(bl // 2):
        span = slice(pair * LANES, (pair + 1) * LANES)
        even, odd = (weight[pl.ds(2 * pair + i, rl, stride=bl), :] for i in range(2))
        maps_ref[0, 0, :, span] = jnp.where(low, even, pltpu.roll(odd, grid, 1))
        maps_ref[0, 1, :, span] = jnp.where(low, pltpu.roll(even, grid, 1), odd)

    half_copy = pltpu.make_async_remote_copy(
        src_ref=maps_ref.at[0], dst_ref=other_map, send_sem=sent, recv_sem=recv_half,
        device_id={"half": 1 - half}, device_id_type=MESH,
    )
    half_copy.start()
    own_rows = pl.ds(pl.multiple_of(32 + 32 * half, 32), 32)
    for rows in (pl.ds(0, 32), own_rows, pl.ds(96, 32)):
        stats[rows] = jnp.zeros((32, LANES), F32)

    def shell_sums(rows_at, values):
        for s in range(shells):
            parts = [jnp.zeros((rl, LANES), F32) for _ in values]
            for pair in range(bl // 2):
                mask = inside[s, pair]
                parts = [part + mask * value[pair] for part, value in zip(parts, values)]
            for at, part in zip(rows_at, parts):
                stats[pl.ds(at + s, 1), :] = jnp.sum(part, axis=0, keepdims=True)

    def tiles(ref, c):
        return [ref[c, :, pair * LANES:(pair + 1) * LANES] for pair in range(bl // 2)]

    mine = [tiles(maps_ref.at[0], c) for c in range(2)]
    shell_sums([32 + 32 * half], [[x * x + y * y for x, y in zip(*mine)]])
    power_copy = pltpu.make_async_remote_copy(
        src_ref=stats.at[own_rows], dst_ref=stats.at[own_rows], send_sem=sent,
        recv_sem=recv_power, device_id={"half": 1 - half}, device_id_type=MESH,
    )
    power_copy.start()
    half_copy.wait_recv()
    theirs = [tiles(other_map, c) for c in range(2)]
    mine = [tiles(maps_ref.at[0], c) for c in range(2)]
    shell_sums([0], [[x * u + y * v for x, y, u, v in zip(*mine, *theirs)]])
    power_copy.wait_recv()
    mine = jnp.sum(stats[...].T, axis=0, keepdims=True)
    total[0] = mine
    stats_in[me] = mine
    for copy in all_to(total, stats_in, recv_stat):
        copy.start()
    whole(stats_in, recv_stat).wait_recv()
    spectra = stats_in[0]
    for n in range(1, N):
        spectra = spectra + stats_in[n]
    spectra_ref[...] = spectra
    rows = sum(sent_rows) + 32 + 2 * (N - 1) + 2 * rl * bl * grid // LANES
    everything = stage_a.at[0, pl.ds(0, rows)]
    pltpu.make_async_remote_copy(
        src_ref=everything, dst_ref=everything, send_sem=sent, recv_sem=recv_half,
        device_id={"half": 1 - half}, device_id_type=MESH,
    ).wait_send()


def finish(shells, maps_in, spectra_ref, counts_ref, maps, power, corr, power_ref, corr_ref, done):
    maps_out = pltpu.make_async_copy(maps_in, maps, done.at[0])
    maps_out.start()
    spectra = spectra_ref[...]
    cross = spectra[:, 0:shells]
    power_first = spectra[:, 32:32 + shells]
    power_second = spectra[:, 64:64 + shells]
    power_ref[0:1, :] = power_first / counts_ref[...]
    power_ref[1:2, :] = power_second / counts_ref[...]
    corr_ref[...] = cross / jnp.sqrt(power_first * power_second + 1e-6)
    small = [
        pltpu.make_async_copy(power_ref, power, done.at[1]),
        pltpu.make_async_copy(corr_ref, corr, done.at[2]),
    ]
    for copy in small:
        copy.start()
    for copy in [maps_out] + small:
        copy.wait()


def solution(mesh):
    R, C = mesh.shape["row"], mesh.shape["col"]
    N = R * C

    def local(particles, orient_bin, tilt_slope, interp_table):
        count, _, grid, plane = particles.shape
        rl, cl, bl = grid // R, plane // C, grid // C
        shells = grid // 2 - 3
        phases = R.bit_length() - 1
        pitch = grid + 8
        bins = interp_table.shape[0]
        steps = C.bit_length() - 1
        nz, n0, n1 = part_rows(rl)
        counts = jnp.asarray(shell_counts(grid)[None], F32)
        vmem, hbm = pl.BlockSpec(memory_space=pltpu.VMEM), pl.BlockSpec(memory_space=pltpu.HBM)
        dma = pltpu.SemaphoreType.DMA
        maps, spectra = pl.pallas_call(
            functools.partial(kernel, (grid, count, R, C, pitch, bins)),
            out_shape=(
                pltpu.VMEM((1, 2, rl, cl), F32),
                pltpu.VMEM((1, LANES), F32),
            ),
            in_specs=[hbm, hbm, hbm, hbm],
            out_specs=(vmem, vmem),
            scratch_shapes=[
                pltpu.VMEM(particles.shape, particles.dtype),
                pltpu.VMEM((bins, grid, grid), interp_table.dtype),
                pltpu.VMEM((bins, 2, grid, grid), interp_table.dtype),
                pltpu.SMEM(orient_bin.shape, jnp.int32),
                pltpu.SMEM(tilt_slope.shape, jnp.int32),
                pltpu.VMEM((count, grid * pitch, LANES), F32),
                pltpu.VMEM((count, C, grid, bl, LANES), F32 if bl % 16 else BF16),
                pltpu.VMEM((C, R, n0 * bl, LANES), F32),
                pltpu.VMEM((C, R, n1 * bl, LANES), F32),
                pltpu.VMEM((C, R, nz * bl, LANES), F32),
                pltpu.VMEM((C, R, n0 * bl, LANES), F32),
                pltpu.VMEM((C, R, n1 * bl, LANES), F32),
                pltpu.VMEM((R, nz * bl, LANES), F32),
                pltpu.VMEM((C, n0 * bl, LANES), F32),
                pltpu.VMEM((C, n1 * bl, LANES), F32),
                pltpu.VMEM((C, R, nz * bl, LANES), F32),
                pltpu.VMEM((2, rl, cl), F32),
                pltpu.VMEM((count * LANES, LANES), BF16),
                pltpu.VMEM((1, 1, LANES), jnp.int32),
                pltpu.VMEM((N, 1, LANES), jnp.int32),
                pltpu.SMEM((N, 1, LANES), jnp.int32),
                pltpu.VMEM((count, R, rl, grid), F32),
                pltpu.VMEM((count, C, bl, grid), F32),
                pltpu.VMEM((C, bl, LANES), F32),
                pltpu.VMEM((bins, rl, grid), F32),
                pltpu.VMEM((bins, bl, LANES), F32),
                pltpu.VMEM((bins, grid, LANES), BF16),
                pltpu.VMEM((rl * bl, LANES), F32),
                pltpu.VMEM((shells, bl // 2, rl, LANES), F32),
                pltpu.VMEM((LANES, LANES), F32),
                pltpu.VMEM((N, 1, LANES), F32),
                pltpu.VMEM((1, 1, LANES), F32),
                dma, dma((phases, 2 * C)), dma((2 * C - 2,)),
                dma((phases,)), dma((C - 1,)),
                dma, dma, dma, dma, dma, dma((count,)), dma, dma, dma, dma,
            ],
            compiler_params=pltpu.CompilerParams(
                collective_id=0, has_side_effects=True, vmem_limit_bytes=VMEM_LIMIT
            ),
        )(orient_bin, tilt_slope, particles, interp_table)
        return pl.pallas_call(
            functools.partial(finish, shells),
            out_shape=(
                jax.ShapeDtypeStruct((1, 2, rl, cl), F32),
                jax.ShapeDtypeStruct((2, shells), F32),
                jax.ShapeDtypeStruct((1, shells), F32),
            ),
            in_specs=[vmem, vmem, vmem],
            out_specs=(hbm, hbm, hbm),
            scratch_shapes=[
                pltpu.VMEM((2, shells), F32), pltpu.VMEM((1, shells), F32), dma((3,)),
            ],
            compiler_params=pltpu.CompilerParams(vmem_limit_bytes=FINISH_LIMIT),
        )(maps, spectra, counts)

    placed = (
        P(("half", "row", "col"), None, None, None),
        P(("half", "row", "col")),
        P(("half", "row", "col"), None),
        P(),
    )
    return jax.shard_map(
        local,
        mesh=mesh,
        in_specs=placed,
        out_specs=(P("half", None, "row", "col"), P(), P("half", None)),
        check_vma=False,
    )
```
